32 devices in a mesh: dp: 4 (over y, z), sp: 8 (over x, core).
Axes of the slice: x: 4, y: 2, z: 2, core: 2. Of those that a mesh axis runs over, the one named last changes fastest.
The devices are a block of a 4x4x8 slice.
Arguments:
- pair_rep: float32 [768, 192, 128], P(('dp', 'sp')), parts along dimension 0
- w_qkvg_s: bfloat16 [128, 512], replicated
- w_bias_s: bfloat16 [4, 128], replicated
- w_out_s: bfloat16 [128, 128], replicated
- w_qkvg_e: bfloat16 [128, 512], replicated
- w_bias_e: bfloat16 [4, 128], replicated
- w_out_e: bfloat16 [128, 128], replicated
- w_one: bfloat16 [128, 512], replicated
- w_two: bfloat16 [512, 128], replicated
Outputs:
- output: float32 [768, 192, 128], P(('dp', 'sp')), parts along dimension 0
There are 4 independent parts. The reference program is written for one: setup_inputs(seed, part) draws one part's arguments, and reference() takes and returns one part's arrays. A program takes and returns all parts, laid end to end along the dimension named above; an argument that names none is the same for every part.
All inputs are finite; a program needn't handle non-finite values.
Results may differ from the reference program's by a relative error of at most 0.0102889.
Values are sent between devices in bfloat16 or wider.
A program may use at most 768 MiB of HBM per device.

```python
import jax
import jax.numpy as jnp
from jax import lax

N = 192
C_Z = 128
HEADS = 4
HEAD_DIM = C_Z // HEADS
HIDDEN = 4 * C_Z
LN_EPS = 1e-5
OUT_SCALE = (N / 16) ** 0.5


def setup_inputs(seed: int = 0, part: int = 0) -> dict:
    root_key = jax.random.key(seed)
    part_key = jax.random.fold_in(root_key, part)
    shared = jax.random.split(jax.random.fold_in(root_key, 65537), 8)
    in_scale = C_Z ** -0.5
    hid_scale = HIDDEN ** -0.5
    pair_rep = jax.random.normal(part_key, (N, N, C_Z), jnp.float32)
    w_qkvg_s = jax.random.normal(shared[0], (C_Z, 4 * C_Z), jnp.float32) * in_scale
    w_bias_s = jax.random.normal(shared[1], (HEADS, C_Z), jnp.float32) * in_scale
    w_out_s = jax.random.normal(shared[2], (C_Z, C_Z), jnp.float32) * (in_scale * OUT_SCALE)
    w_qkvg_e = jax.random.normal(shared[3], (C_Z, 4 * C_Z), jnp.float32) * in_scale
    w_bias_e = jax.random.normal(shared[4], (HEADS, C_Z), jnp.float32) * in_scale
    w_out_e = jax.random.normal(shared[5], (C_Z, C_Z), jnp.float32) * (in_scale * OUT_SCALE)
    w_one = jax.random.normal(shared[6], (C_Z, HIDDEN), jnp.float32) * in_scale
    w_two = jax.random.normal(shared[7], (HIDDEN, C_Z), jnp.float32) * hid_scale
    return {
        "pair_rep": pair_rep,
        "w_qkvg_s": w_qkvg_s.astype(jnp.bfloat16),
        "w_bias_s": w_bias_s.astype(jnp.bfloat16),
        "w_out_s": w_out_s.astype(jnp.bfloat16),
        "w_qkvg_e": w_qkvg_e.astype(jnp.bfloat16),
        "w_bias_e": w_bias_e.astype(jnp.bfloat16),
        "w_out_e": w_out_e.astype(jnp.bfloat16),
        "w_one": w_one.astype(jnp.bfloat16),
        "w_two": w_two.astype(jnp.bfloat16),
    }


def layer_norm(values):
    vals_f = values.astype(jnp.float32)
    mean_c = jnp.mean(vals_f, axis=-1, keepdims=True)
    centered = vals_f - mean_c
    variance = jnp.mean(centered * centered, axis=-1, keepdims=True)
    return (centered * lax.rsqrt(variance + LN_EPS)).astype(jnp.bfloat16)


def bias_table(pair_in, w_bias):
    def one_row(row_in):
        return jnp.dot(layer_norm(row_in), w_bias.T, preferred_element_type=jnp.float32).astype(jnp.bfloat16)
    return jnp.transpose(lax.map(one_row, pair_in), (2, 0, 1))


def row_update(row_in, bias_full, w_qkvg, w_out):
    seq_len = row_in.shape[0]
    projected = jnp.dot(layer_norm(row_in), w_qkvg, preferred_element_type=jnp.float32)
    split_shape = (seq_len, HEADS, HEAD_DIM)
    queries = projected[:, :C_Z].astype(jnp.bfloat16).reshape(split_shape).astype(jnp.float32)
    key_vecs = projected[:, C_Z:2 * C_Z].astype(jnp.bfloat16).reshape(split_shape).astype(jnp.float32)
    val_vecs = projected[:, 2 * C_Z:3 * C_Z].astype(jnp.bfloat16).reshape(split_shape).astype(jnp.float32)
    gate_vals = jax.nn.sigmoid(projected[:, 3 * C_Z:]).reshape(split_shape)
    scores = jnp.einsum('jhd,khd->hjk', queries, key_vecs) * HEAD_DIM ** -0.5 + bias_full.astype(jnp.float32)
    attn_prob = jax.nn.softmax(scores, axis=-1).astype(jnp.bfloat16).astype(jnp.float32)
    attn_out = jnp.einsum('hjk,khd->jhd', attn_prob, val_vecs)
    gated_out = (attn_out * gate_vals).astype(jnp.bfloat16).reshape(seq_len, C_Z)
    return jnp.dot(gated_out, w_out, preferred_element_type=jnp.float32)


def tri_attention(pair_in, w_qkvg, w_bias, w_out):
    bias_full = bias_table(pair_in, w_bias)

    def one_row(row_in):
        return row_update(row_in, bias_full, w_qkvg, w_out)
    return lax.map(one_row, pair_in)


def reference(pair_rep, w_qkvg_s, w_bias_s, w_out_s, w_qkvg_e, w_bias_e, w_out_e, w_one, w_two):
    pair_one = pair_rep + tri_attention(pair_rep, w_qkvg_s, w_bias_s, w_out_s)
    pair_trans = jnp.swapaxes(pair_one.astype(jnp.bfloat16), 0, 1)
    end_upd = tri_attention(pair_trans, w_qkvg_e, w_bias_e, w_out_e)

    def finish_row(row_pair):
        trans_row, upd_row = row_pair
        pair_two = trans_row.astype(jnp.float32) + upd_row
        hidden = jax.nn.relu(jnp.dot(layer_norm(pair_two), w_one, preferred_element_type=jnp.float32))
        trans_out = jnp.dot(hidden.astype(jnp.bfloat16), w_two, preferred_element_type=jnp.float32)
        return (upd_row + trans_out).astype(jnp.bfloat16)

    delta_trans = lax.map(finish_row, (pair_trans, end_upd))
    return pair_one + jnp.swapaxes(delta_trans, 0, 1).astype(jnp.float32)
```

```python
import functools

import jax
import jax.numpy as jnp
from jax import lax
from jax.experimental import pallas as pl
from jax.experimental.pallas import tpu as pltpu
from jax.sharding import PartitionSpec as P

LN_EPS = 1e-5
LANES = 128
F32, BF16 = jnp.float32, jnp.bfloat16


def layer_norm(vals):
    mean = jnp.mean(vals, axis=-1, keepdims=True)
    centered = vals - mean
    var = jnp.mean(centered * centered, axis=-1, keepdims=True)
    return (centered * lax.rsqrt(var + LN_EPS)).astype(BF16)


def mm(lhs, rhs, contract=((1,), (0,))):
    return lax.dot_general(lhs, rhs, (contract, ((), ())), preferred_element_type=F32)


def loop(count, body, unroll=1):
    def step(idx, carry):
        for sub in range(unroll):
            body(idx * unroll + sub)
        return carry

    lax.fori_loop(0, count // unroll, step, 0)


def kernel(cfg, z_ref, wqs_ref, wbs_ref, wos_ref, wqe_ref, wbe_ref, woe_ref, w1_ref, w2_ref, out_ref,
           z1, flat, norm, w_t, w_b, qmask, v_t, gate_t, keys, bias_rows, bias_out, bias_in, bias_t,
           h_out, h_in, d_out, d_in, out_sem, bias_sem, h_sem, d_sem):
    group, rows, seq, chan, heads, axis = cfg
    dim = chan // heads
    me = lax.axis_index(axis)
    tail = seq - LANES
    sub = rows // 8
    scale = dim ** -0.5

    barrier = pltpu.get_barrier_semaphore()
    for off in range(1, group):
        pl.semaphore_signal(barrier, inc=1, device_id={axis: lax.rem(me + off, group)}, device_id_type=pl.DeviceIdType.MESH)

    lane = lax.broadcasted_iota(jnp.int32, (1, LANES), 1)
    low = lane < tail

    def doubled(rows_in):
        return jnp.concatenate([rows_in, rows_in[LANES:seq]], axis=0)

    def peers(start):
        for off in range(1, group):
            start(lax.rem(me + off, group))

    def remote(src, dst, recv, dst_dev):
        return pltpu.make_async_remote_copy(src_ref=src, dst_ref=dst, send_sem=out_sem, recv_sem=recv,
                                            device_id={axis: dst_dev}, device_id_type=pl.DeviceIdType.MESH)

    def wait_recv(ref, sem):
        part = ref.at[pl.ds(0, group - 1)]
        pltpu.make_async_remote_copy(src_ref=part, dst_ref=part, send_sem=out_sem, recv_sem=sem,
                                     device_id={axis: me}, device_id_type=pl.DeviceIdType.MESH).wait_recv()

    def wait_send(ref):
        part = ref.at[pl.ds(0, group - 1)]
        pltpu.make_async_remote_copy(src_ref=part, dst_ref=part, send_sem=out_sem, recv_sem=out_sem,
                                     device_id={axis: me}, device_id_type=pl.DeviceIdType.MESH).wait_send()

    def load_weights(wq_ref, wb_ref):
        for dst, src in ((0, 0), (1, 2), (2, 3)):
            w_t[pl.ds(dst * chan, chan), :] = wq_ref[:, pl.ds(src * chan, chan)].T
        w_b[...] = jnp.zeros(w_b.shape, w_b.dtype)
        w_b[pl.ds(0, heads), :] = wb_ref[...].astype(F32)

    def norm_and_bias(read, phase, first_send):
        wb = w_b[...].astype(BF16)

        def row(r):
            u = layer_norm(read(r))
            norm[r] = u
            b = mm(wb, doubled(u), ((1,), (1,)))
            for pair in range(heads // 2):
                b0, b1 = b[2 * pair:2 * pair + 1], b[2 * pair + 1:2 * pair + 2]
                bias_rows[pair, 0, pl.ds(r, 1), :] = b0[:, :LANES]
                bias_rows[pair, 1, pl.ds(r, 1), :] = b1[:, :LANES]
                bias_rows[pair, 2, pl.ds(r, 1), :] = jnp.where(low, b0[:, LANES:], b1[:, LANES:])

        loop(rows, row, 4)
        rounded = bias_rows[...].astype(BF16).reshape(bias_out.shape[1:])
        bias_out[phase] = rounded
        bias_in[phase, me] = rounded
        first_send()
        peers(lambda d: remote(bias_out.at[phase], bias_in.at[phase, me], bias_sem.at[phase], d).start())

    def project(wq_ref):
        def row(r):
            u = norm[r]
            keys[r] = mm(u, wq_ref[:, pl.ds(chan, chan)]).astype(BF16)
            proj = mm(w_t[...], doubled(u), ((1,), (1,)))
            q, v, gl = proj[:chan], proj[chan:2 * chan], proj[2 * chan:]
            qmask[r, :, pl.ds(0, LANES)] = q[:, :LANES].astype(BF16)
            for h in range(heads):
                part = q[h * dim:(h + 1) * dim, LANES:]
                keep = low if h % 2 == 0 else jnp.logical_not(low)
                qmask[r, pl.ds(h * dim, dim), pl.ds(LANES, LANES)] = jnp.where(keep, part, 0.0).astype(BF16)
            v_t[r] = v[:, :seq].astype(BF16)
            gate_t[r] = jax.nn.sigmoid(gl)

        loop(rows, row, 2)

    def spread_bias(phase):
        wait_recv(bias_in.at[phase], bias_sem.at[phase])
        for pair in range(heads // 2):
            t0, t1, t2 = [doubled(bias_in[phase, :, pair, t].astype(F32).reshape(group * rows, LANES)).T for t in range(3)]
            even = jnp.concatenate([t0, t2[:tail]], axis=0)
            odd = jnp.concatenate([t1, t2[tail:]], axis=0)
            bias_t[pair, :, pl.ds(0, LANES)] = even[:, :LANES]
            bias_t[pair, :, pl.ds(LANES, LANES)] = odd[:, :LANES]
            bias_t[2, :, pl.ds(pair * LANES, LANES)] = jnp.where(low, even[:, LANES:], odd[:, LANES:])

    def attention(r, wo):
        key, qm, vt, gate = keys[r], qmask[r], v_t[r], gate_t[r]
        zero = jnp.zeros((dim, LANES), BF16)
        zero2 = jnp.zeros((2 * dim, LANES), BF16)
        zero4 = jnp.zeros((2 * dim, 2 * LANES), BF16)

        def pair_rhs(pair):
            a = qm[2 * pair * dim:(2 * pair + 1) * dim, :LANES]
            b = qm[(2 * pair + 1) * dim:(2 * pair + 2) * dim, :LANES]
            return jnp.concatenate([jnp.concatenate([a, zero], axis=1), jnp.concatenate([zero, b], axis=1)], axis=0)

        rhs = [jnp.concatenate([pair_rhs(0), zero4], axis=0), jnp.concatenate([zero4, pair_rhs(1)], axis=0),
               jnp.concatenate([jnp.concatenate([qm[:2 * dim, LANES:], zero2], axis=1),
                                jnp.concatenate([zero2, qm[2 * dim:, LANES:]], axis=1)], axis=0)]
        values = [vt[:2 * dim], vt[2 * dim:], vt]
        mixed = []
        for t in range(3):
            s = mm(key, rhs[t]) * scale + bias_t[t]
            e = jnp.exp(s - jnp.max(s, axis=0, keepdims=True))
            total = jnp.sum(e, axis=0, keepdims=True)
            mixed.append(mm(values[t], e.astype(BF16)) * (1.0 / total))
        main = jnp.concatenate([mixed[0][:dim, :LANES], mixed[0][dim:, LANES:], mixed[1][:dim, :LANES], mixed[1][dim:, LANES:]], axis=0)
        rest = []
        for h in range(heads):
            part = mixed[2][h * dim:(h + 1) * dim, (h // 2) * LANES:(h // 2 + 1) * LANES] * gate[h * dim:(h + 1) * dim, LANES:]
            rest.append(jnp.where(low if h % 2 == 0 else jnp.logical_not(low), part, 0.0))
        main = (main * gate[:, :LANES]).astype(BF16)
        rest = jnp.concatenate(rest, axis=0).astype(BF16)
        upd = mm(jnp.concatenate([main.T, rest.T], axis=0), wo)
        return jnp.concatenate([upd[:LANES], upd[LANES:LANES + tail] + upd[LANES + tail:]], axis=0)

    def send_row(r, src, dst, sem):
        mine = pl.ds(me * sub, sub)
        dst[me, r] = src[r, mine]
        peers(lambda d: remote(src.at[r, pl.ds(d * sub, sub)], dst.at[me, r], sem, d).start())

    def unpack(src):
        def part(d):
            flat[pl.ds(d * rows * rows, rows * rows), :] = src[d].astype(F32).reshape(rows * rows, chan)

        loop(group, part)

    load_weights(wqs_ref, wbs_ref)
    norm_and_bias(lambda r: z_ref[r], 0, lambda: pl.semaphore_wait(barrier, group - 1))
    project(wqs_ref)
    spread_bias(0)

    def start_row(r):
        new = z_ref[r] + attention(r, wos_ref[...])
        z1[r] = new
        h_out[r] = new.astype(BF16).reshape(seq // 8, 8, chan)
        send_row(r, h_out, h_in, h_sem)

    loop(rows, start_row, 2)

    load_weights(wqe_ref, wbe_ref)
    wait_recv(h_in, h_sem)
    unpack(h_in)
    column = lambda c: flat[pl.ds(c, seq, stride=rows), :]
    norm_and_bias(column, 1, lambda: None)
    project(wqe_ref)
    spread_bias(1)

    def end_row(c):
        upd = attention(c, woe_ref[...])
        hidden = jnp.maximum(mm(layer_norm(column(c) + upd), w1_ref[...]), 0.0).astype(BF16)
        delta = upd + mm(hidden, w2_ref[...])
        d_out[c] = delta.astype(BF16).reshape(seq // 8, 8, chan)
        send_row(c, d_out, d_in, d_sem)

    loop(rows, end_row, 2)
    wait_recv(d_in, d_sem)
    unpack(d_in)

    def final(r):
        out_ref[r] = z1[r] + flat[pl.ds(r, seq, stride=rows), :]

    loop(rows, final, 2)
    for phase in range(2):
        for _ in range(group - 1):
            remote(bias_out.at[phase], bias_in.at[phase, me], bias_sem.at[phase], me).wait_send()
    wait_send(h_in)
    wait_send(d_in)


def solution(mesh):
    axis = 'sp'
    group = mesh.shape[axis]
    row_spec = P(('dp', 'sp'), None, None)

    def local_fn(pair_loc, w_qkvg_s, w_bias_s, w_out_s, w_qkvg_e, w_bias_e, w_out_e, w_one, w_two):
        rows, seq, chan = pair_loc.shape
        heads = w_bias_s.shape[0]
        sub = rows // 8
        packed = 2 * LANES
        vmem = pl.BlockSpec(memory_space=pltpu.VMEM)
        scratch = [
            pltpu.VMEM((rows, seq, chan), F32),
            pltpu.VMEM((rows * seq, chan), F32),
            pltpu.VMEM((rows, seq, chan), BF16),
            pltpu.VMEM((3 * chan, chan), BF16),
            pltpu.VMEM((16, chan), F32),
            pltpu.VMEM((rows, chan, packed), BF16),
            pltpu.VMEM((rows, chan, seq), BF16),
            pltpu.VMEM((rows, chan, packed), F32),
            pltpu.VMEM((rows, seq, chan), BF16),
            pltpu.VMEM((heads // 2, 3, rows, LANES), F32),
            pltpu.VMEM((2, heads // 2, 3, sub, 8, LANES), BF16),
            pltpu.VMEM((2, group, heads // 2, 3, sub, 8, LANES), BF16),
            pltpu.VMEM((3, seq, packed), F32),
            pltpu.VMEM((rows, seq // 8, 8, chan), BF16),
            pltpu.VMEM((group, rows, sub, 8, chan), BF16),
            pltpu.VMEM((rows, seq // 8, 8, chan), BF16),
            pltpu.VMEM((group, rows, sub, 8, chan), BF16),
            pltpu.SemaphoreType.DMA,
            pltpu.SemaphoreType.DMA((2,)),
            pltpu.SemaphoreType.DMA,
            pltpu.SemaphoreType.DMA,
        ]
        return pl.pallas_call(
            functools.partial(kernel, (group, rows, seq, chan, heads, axis)),
            out_shape=jax.ShapeDtypeStruct(pair_loc.shape, F32),
            in_specs=[vmem] * 9,
            out_specs=vmem,
            scratch_shapes=scratch,
            compiler_params=pltpu.CompilerParams(collective_id=0, has_side_effects=True, vmem_limit_bytes=60 * 2 ** 20),
        )(pair_loc, w_qkvg_s, w_bias_s, w_out_s, w_qkvg_e, w_bias_e, w_out_e, w_one, w_two)

    return jax.shard_map(local_fn, mesh=mesh, in_specs=(row_spec, P(), P(), P(), P(), P(), P(), P(), P()), out_specs=row_spec, check_vma=False)
```

```python
import functools

import jax
import jax.numpy as jnp
from jax import lax
from jax.experimental import pallas as pl
from jax.experimental.pallas import tpu as pltpu
from jax.sharding import PartitionSpec as P

LN_EPS = 1e-5
LANES = 128
SEND = 2
F32, BF16 = jnp.float32, jnp.bfloat16


def layer_norm(vals):
    mean = jnp.mean(vals, axis=-1, keepdims=True)
    centered = vals - mean
    var = jnp.mean(centered * centered, axis=-1, keepdims=True)
    return (centered * lax.rsqrt(var + LN_EPS)).astype(BF16)


def mm(lhs, rhs, contract=((1,), (0,))):
    return lax.dot_general(lhs, rhs, (contract, ((), ())), preferred_element_type=F32)


def loop(count, body, unroll=1):
    def step(idx, carry):
        for sub in range(unroll):
            body(idx * unroll + sub)
        return carry

    lax.fori_loop(0, count // unroll, step, 0)


def kernel(cfg, z_ref, wqs_ref, wbs_ref, wos_ref, wqe_ref, wbe_ref, woe_ref, w1_ref, w2_ref, out_ref,
           z1, flat, norm, w_t, w_b, qmask, v_t, gate_t, keys, bias_rows, bias_out, bias_in, bias_t, scores, tops, mixed, upds, normed,
           h_out, h_in, d_out, d_in, out_sem, bias_sem, h_sem, d_sem):
    group, rows, seq, chan, heads, axis = cfg
    dim = chan // heads
    me = lax.axis_index(axis)
    tail = seq - LANES
    sub = rows // 8
    scale = dim ** -0.5

    barrier = pltpu.get_barrier_semaphore()
    for off in range(1, group):
        pl.semaphore_signal(barrier, inc=1, device_id={axis: lax.rem(me + off, group)}, device_id_type=pl.DeviceIdType.MESH)

    lane = lax.broadcasted_iota(jnp.int32, (1, LANES), 1)
    low = lane < tail

    def doubled(rows_in):
        return jnp.concatenate([rows_in, rows_in[LANES:seq]], axis=0)

    def peers(start):
        for off in range(1, group):
            start(lax.rem(me + off, group))

    def remote(src, dst, recv, dst_dev):
        return pltpu.make_async_remote_copy(src_ref=src, dst_ref=dst, send_sem=out_sem, recv_sem=recv,
                                            device_id={axis: dst_dev}, device_id_type=pl.DeviceIdType.MESH)

    def wait_recv(ref, sem):
        part = ref.at[pl.ds(0, group - 1)]
        pltpu.make_async_remote_copy(src_ref=part, dst_ref=part, send_sem=out_sem, recv_sem=sem,
                                     device_id={axis: me}, device_id_type=pl.DeviceIdType.MESH).wait_recv()

    def wait_send(ref):
        part = ref.at[pl.ds(0, group - 1)]
        pltpu.make_async_remote_copy(src_ref=part, dst_ref=part, send_sem=out_sem, recv_sem=out_sem,
                                     device_id={axis: me}, device_id_type=pl.DeviceIdType.MESH).wait_send()

    def load_weights(wq_ref, wb_ref):
        for dst, src in ((0, 0), (1, 2), (2, 3)):
            w_t[pl.ds(dst * chan, chan), :] = wq_ref[:, pl.ds(src * chan, chan)].T
        w_b[...] = jnp.zeros(w_b.shape, w_b.dtype)
        w_b[pl.ds(0, heads), :] = wb_ref[...].astype(F32)

    def norm_and_bias(read, phase, first_send):
        wb = w_b[...].astype(BF16)

        def row(r):
            u = layer_norm(read(r))
            norm[r] = u
            b = mm(wb, doubled(u), ((1,), (1,)))
            for pair in range(heads // 2):
                b0, b1 = b[2 * pair:2 * pair + 1], b[2 * pair + 1:2 * pair + 2]
                bias_rows[pair, 0, pl.ds(r, 1), :] = b0[:, :LANES]
                bias_rows[pair, 1, pl.ds(r, 1), :] = b1[:, :LANES]
                bias_rows[pair, 2, pl.ds(r, 1), :] = jnp.where(low, b0[:, LANES:], b1[:, LANES:])

        loop(rows, row, 4)
        rounded = bias_rows[...].astype(BF16).reshape(bias_out.shape[1:])
        bias_out[phase] = rounded
        bias_in[phase, me] = rounded
        first_send()
        peers(lambda d: remote(bias_out.at[phase], bias_in.at[phase, me], bias_sem.at[phase], d).start())

    def project(wq_ref):
        def row(r):
            u = norm[r]
            keys[r] = mm(u, wq_ref[:, pl.ds(chan, chan)]).astype(BF16)
            proj = mm(w_t[...], doubled(u), ((1,), (1,)))
            q, v, gl = proj[:chan], proj[chan:2 * chan], proj[2 * chan:]
            qmask[r, :, pl.ds(0, LANES)] = q[:, :LANES].astype(BF16)
            for h in range(heads):
                part = q[h * dim:(h + 1) * dim, LANES:]
                keep = low if h % 2 == 0 else jnp.logical_not(low)
                qmask[r, pl.ds(h * dim, dim), pl.ds(LANES, LANES)] = jnp.where(keep, part, 0.0).astype(BF16)
            v_t[r] = v[:, :seq].astype(BF16)
            gate_t[r] = jax.nn.sigmoid(gl)

        loop(rows, row, 2)

    def spread_bias(phase):
        wait_recv(bias_in.at[phase], bias_sem.at[phase])
        for pair in range(heads // 2):
            t0, t1, t2 = [doubled(bias_in[phase, :, pair, t].astype(F32).reshape(group * rows, LANES)).T for t in range(3)]
            even = jnp.concatenate([t0, t2[:tail]], axis=0)
            odd = jnp.concatenate([t1, t2[tail:]], axis=0)
            bias_t[pair, :, pl.ds(0, LANES)] = even[:, :LANES]
            bias_t[pair, :, pl.ds(LANES, LANES)] = odd[:, :LANES]
            bias_t[2, :, pl.ds(pair * LANES, LANES)] = jnp.where(low, even[:, LANES:], odd[:, LANES:])

    zero = jnp.zeros((dim, LANES), BF16)
    zero2 = jnp.zeros((2 * dim, LANES), BF16)
    zero4 = jnp.zeros((2 * dim, 2 * LANES), BF16)

    def query_tile(r, t):
        if t == 2:
            top = jnp.concatenate([qmask[r, pl.ds(0, 2 * dim), pl.ds(LANES, LANES)], zero2], axis=1)
            bottom = jnp.concatenate([zero2, qmask[r, pl.ds(2 * dim, 2 * dim), pl.ds(LANES, LANES)]], axis=1)
            return jnp.concatenate([top, bottom], axis=0)
        first = qmask[r, pl.ds(2 * t * dim, dim), pl.ds(0, LANES)]
        second = qmask[r, pl.ds((2 * t + 1) * dim, dim), pl.ds(0, LANES)]
        pair = jnp.concatenate([jnp.concatenate([first, zero], axis=1), jnp.concatenate([zero, second], axis=1)], axis=0)
        return jnp.concatenate([pair, zero4] if t == 0 else [zero4, pair], axis=0)

    def score_tile(r, t):
        s = mm(keys[r], query_tile(r, t)) * scale + bias_t[t]
        scores[t] = s
        tops[t] = jnp.max(s, axis=0, keepdims=True)

    def mix_tile(r, t):
        e = jnp.exp(scores[t] - tops[t])
        total = jnp.sum(e, axis=0, keepdims=True)
        values = v_t[r] if t == 2 else v_t[r, pl.ds(2 * t * dim, 2 * dim), :]
        o = mm(values, e.astype(BF16)) * (1.0 / total)
        if t < 2:
            for h in (2 * t, 2 * t + 1):
                part = o[(h % 2) * dim:(h % 2 + 1) * dim, (h % 2) * LANES:(h % 2 + 1) * LANES]
                mixed[pl.ds(h * dim, dim), pl.ds(0, LANES)] = (part * gate_t[r, pl.ds(h * dim, dim), pl.ds(0, LANES)]).astype(BF16)
        else:
            for h in range(heads):
                part = o[h * dim:(h + 1) * dim, (h // 2) * LANES:(h // 2 + 1) * LANES] * gate_t[r, pl.ds(h * dim, dim), pl.ds(LANES, LANES)]
                mixed[pl.ds(h * dim, dim), pl.ds(LANES, LANES)] = jnp.where(low if h % 2 == 0 else jnp.logical_not(low), part, 0.0).astype(BF16)

    def merge_heads(wo):
        upd = mm(mixed[...].T, wo)
        return jnp.concatenate([upd[:LANES], upd[LANES:LANES + tail] + upd[LANES + tail:]], axis=0)

    def pipeline(steps, lag):
        def step(idx, carry):
            steps(idx, lambda back: jnp.clip(idx - back, 0, rows - 1))
            return carry

        lax.fori_loop(0, rows + lag, step, 0)

    def send_rows(last, src, dst, sem):
        @pl.when(jnp.logical_and(last >= 0, lax.rem(last, SEND) == SEND - 1))
        def _():
            some = pl.ds(last - (SEND - 1), SEND)
            dst[me, some] = src[some, pl.ds(me * sub, sub)]
            peers(lambda d: remote(src.at[some, pl.ds(d * sub, sub)], dst.at[me, some], sem, d).start())

    def unpack(src):
        def part(d):
            flat[pl.ds(d * rows * rows, rows * rows), :] = src[d].astype(F32).reshape(rows * rows, chan)

        loop(group, part)

    load_weights(wqs_ref, wbs_ref)
    norm_and_bias(lambda r: z_ref[r], 0, lambda: pl.semaphore_wait(barrier, group - 1))
    project(wqs_ref)
    spread_bias(0)

    def start_step(idx, at):
        r = at(2)
        z_new = z_ref[r] + merge_heads(wos_ref[...])
        z1[r] = z_new
        h_out[r] = z_new.astype(BF16).reshape(seq // 8, 8, chan)
        for t in range(3):
            mix_tile(at(1), t)
            score_tile(at(0), t)
        send_rows(idx - 2, h_out, h_in, h_sem)

    pipeline(start_step, 2)

    load_weights(wqe_ref, wbe_ref)
    wait_recv(h_in, h_sem)
    unpack(h_in)
    column = lambda c: flat[pl.ds(c, seq, stride=rows), :]
    norm_and_bias(column, 1, lambda: None)
    project(wqe_ref)
    spread_bias(1)

    def end_step(idx, at):
        hidden = jnp.maximum(mm(normed[...], w1_ref[...]), 0.0).astype(BF16)
        d_out[at(3)] = (upds[...] + mm(hidden, w2_ref[...])).astype(BF16).reshape(seq // 8, 8, chan)
        upd = merge_heads(woe_ref[...])
        upds[...] = upd
        normed[...] = layer_norm(column(at(2)) + upd)
        for t in range(3):
            mix_tile(at(1), t)
            score_tile(at(0), t)
        send_rows(idx - 3, d_out, d_in, d_sem)

    pipeline(end_step, 3)
    wait_recv(d_in, d_sem)
    unpack(d_in)

    def final(r):
        out_ref[r] = z1[r] + flat[pl.ds(r, seq, stride=rows), :]

    loop(rows, final, 2)
    for phase in range(2):
        for _ in range(group - 1):
            remote(bias_out.at[phase], bias_in.at[phase, me], bias_sem.at[phase], me).wait_send()
    wait_send(h_in)
    wait_send(d_in)


def solution(mesh):
    axis = 'sp'
    group = mesh.shape[axis]
    row_spec = P(('dp', 'sp'), None, None)

    def local_fn(pair_loc, w_qkvg_s, w_bias_s, w_out_s, w_qkvg_e, w_bias_e, w_out_e, w_one, w_two):
        rows, seq, chan = pair_loc.shape
        heads = w_bias_s.shape[0]
        sub = rows // 8
        packed = 2 * LANES
        vmem = pl.BlockSpec(memory_space=pltpu.VMEM)
        scratch = [
            pltpu.VMEM((rows, seq, chan), F32),
            pltpu.VMEM((rows * seq, chan), F32),
            pltpu.VMEM((rows, seq, chan), BF16),
            pltpu.VMEM((3 * chan, chan), BF16),
            pltpu.VMEM((16, chan), F32),
            pltpu.VMEM((rows, chan, packed), BF16),
            pltpu.VMEM((rows, chan, seq), BF16),
            pltpu.VMEM((rows, chan, packed), F32),
            pltpu.VMEM((rows, seq, chan), BF16),
            pltpu.VMEM((heads // 2, 3, rows, LANES), F32),
            pltpu.VMEM((2, heads // 2, 3, sub, 8, LANES), BF16),
            pltpu.VMEM((2, group, heads // 2, 3, sub, 8, LANES), BF16),
            pltpu.VMEM((3, seq, packed), F32),
            pltpu.VMEM((3, seq, packed), F32),
            pltpu.VMEM((3, 1, packed), F32),
            pltpu.VMEM((chan, packed), BF16),
            pltpu.VMEM((seq, chan), F32),
            pltpu.VMEM((seq, chan), BF16),
            pltpu.VMEM((rows, seq // 8, 8, chan), BF16),
            pltpu.VMEM((group, rows, sub, 8, chan), BF16),
            pltpu.VMEM((rows, seq // 8, 8, chan), BF16),
            pltpu.VMEM((group, rows, sub, 8, chan), BF16),
            pltpu.SemaphoreType.DMA,
            pltpu.SemaphoreType.DMA((2,)),
            pltpu.SemaphoreType.DMA,
            pltpu.SemaphoreType.DMA,
        ]
        return pl.pallas_call(
            functools.partial(kernel, (group, rows, seq, chan, heads, axis)),
            out_shape=jax.ShapeDtypeStruct(pair_loc.shape, F32),
            in_specs=[vmem] * 9,
            out_specs=vmem,
            scratch_shapes=scratch,
            compiler_params=pltpu.CompilerParams(collective_id=0, has_side_effects=True, vmem_limit_bytes=60 * 2 ** 20),
        )(pair_loc, w_qkvg_s, w_bias_s, w_out_s, w_qkvg_e, w_bias_e, w_out_e, w_one, w_two)

    return jax.shard_map(local_fn, mesh=mesh, in_specs=(row_spec, P(), P(), P(), P(), P(), P(), P(), P()), out_specs=row_spec, check_vma=False)
```

```python
import functools

import jax
import jax.numpy as jnp
from jax import lax
from jax.experimental import pallas as pl
from jax.experimental.pallas import tpu as pltpu
from jax.sharding import PartitionSpec as P

LN_EPS = 1e-5
LANES = 128
SEND = 2
F32, BF16 = jnp.float32, jnp.bfloat16


def layer_norm(vals):
    mean = jnp.mean(vals, axis=-1, keepdims=True)
    centered = vals - mean
    var = jnp.mean(centered * centered, axis=-1, keepdims=True)
    return (centered * lax.rsqrt(var + LN_EPS)).astype(BF16)


def mm(lhs, rhs, contract=((1,), (0,))):
    return lax.dot_general(lhs, rhs, (contract, ((), ())), preferred_element_type=F32)


def loop(count, body, unroll=1):
    def step(idx, carry):
        for sub in range(unroll):
            body(idx * unroll + sub)
        return carry

    lax.fori_loop(0, count // unroll, step, 0)


def kernel(cfg, z_hbm, wqs_hbm, wbs_hbm, wos_hbm, wqe_hbm, wbe_hbm, woe_hbm, w1_hbm, w2_hbm, out_ref,
           z_ref, wqs_ref, wbs_ref, wos_ref, wqe_ref, wbe_ref, woe_ref, w1_ref, w2_ref,
           flat, norm, norm_b, w_t, w_b, qmask, v_t, gate_t, keys, bias_rows, bias_out, bias_in, bias_t, scores, tops, mixed, upds, normed,
           h_out, h_in, d_out, d_in, z_sem, w_sem, out_sem, bias_sem, h_sem, d_sem):
    group, rows, seq, chan, heads, axis = cfg
    dim = chan // heads
    me = lax.axis_index(axis)
    tail = seq - LANES
    sub = rows // 8
    scale = dim ** -0.5
    early = LANES // group

    loads = []
    pairs = ((wqs_hbm, wqs_ref), (wbs_hbm, wbs_ref), (wos_hbm, wos_ref), (wqe_hbm, wqe_ref),
             (wbe_hbm, wbe_ref), (woe_hbm, woe_ref), (w1_hbm, w1_ref), (w2_hbm, w2_ref))
    z_copy = lambda g: pltpu.make_async_copy(z_hbm.at[pl.ds(g * 8, 8)], z_ref.at[pl.ds(g * 8, 8)], z_sem.at[g])
    for g in range(sub):
        z_copy(g).start()
    for i, (src, dst) in enumerate(pairs):
        loads.append(pltpu.make_async_copy(src, dst, w_sem.at[i]))
        loads[i].start()

    barrier = pltpu.get_barrier_semaphore()
    for off in range(1, group):
        pl.semaphore_signal(barrier, inc=1, device_id={axis: lax.rem(me + off, group)}, device_id_type=pl.DeviceIdType.MESH)

    lane = lax.broadcasted_iota(jnp.int32, (1, LANES), 1)
    low = lane < tail

    def doubled(rows_in):
        return jnp.concatenate([rows_in, rows_in[LANES:seq]], axis=0)

    def peers(start):
        for off in range(1, group):
            start(lax.rem(me + off, group))

    def remote(src, dst, recv, dst_dev):
        return pltpu.make_async_remote_copy(src_ref=src, dst_ref=dst, send_sem=out_sem, recv_sem=recv,
                                            device_id={axis: dst_dev}, device_id_type=pl.DeviceIdType.MESH)

    def wait_recv(part, sem):
        pltpu.make_async_remote_copy(src_ref=part, dst_ref=part, send_sem=out_sem, recv_sem=sem,
                                     device_id={axis: me}, device_id_type=pl.DeviceIdType.MESH).wait_recv()

    def wait_send(part):
        pltpu.make_async_remote_copy(src_ref=part, dst_ref=part, send_sem=out_sem, recv_sem=out_sem,
                                     device_id={axis: me}, device_id_type=pl.DeviceIdType.MESH).wait_send()

    others = pl.ds(0, group - 1)

    def load_weights(wq_ref, wb_ref):
        for dst, src in ((0, 0), (1, 2), (2, 3)):
            w_t[pl.ds(dst * chan, chan), :] = wq_ref[:, pl.ds(src * chan, chan)].T
        w_b[...] = jnp.zeros(w_b.shape, w_b.dtype)
        w_b[pl.ds(0, heads), :] = wb_ref[...].astype(F32)

    def put_bias(c, tile, even, odd):
        if tile == 0:
            for pair in range(heads // 2):
                bias_rows[pair, 0, pl.ds(c, 1), :] = even[2 * pair:2 * pair + 1]
                bias_rows[pair, 1, pl.ds(c, 1), :] = even[2 * pair + 1:2 * pair + 2]
        else:
            for pair in range(heads // 2):
                bias_rows[pair, 2, pl.ds(c, 1), :] = jnp.where(low, even[2 * pair:2 * pair + 1], odd[2 * pair + 1:2 * pair + 2])

    def send_bias(phase, tiles, some):
        rounded = bias_rows[:, tiles, some].astype(BF16).reshape(heads // 2, tiles.size, some.size // 8, 8, LANES)
        part = pl.ds(some.start // 8, some.size // 8)
        bias_out[phase, :, tiles, part] = rounded
        bias_in[phase, me, :, tiles, part] = rounded
        peers(lambda d: remote(bias_out.at[phase, :, tiles, part], bias_in.at[phase, me, :, tiles, part], bias_sem.at[phase], d).start())

    def start_norm():
        wb = w_b[...].astype(BF16)
        for g in range(sub):
            z_copy(g).wait()

            def row(i):
                r = g * 8 + i
                u = layer_norm(z_ref[r])
                norm[r] = u
                b = mm(wb, doubled(u), ((1,), (1,)))
                put_bias(r, 0, b[:, :LANES], None)
                put_bias(r, 1, b[:, LANES:], b[:, LANES:])

            loop(8, row, 4)
            if g == 0:
                pl.semaphore_wait(barrier, group - 1)
            send_bias(0, pl.ds(0, 3), pl.ds(g * 8, 8))

    def put_projected(c, proj, lo, width):
        q, v, gl = proj[:chan], proj[chan:2 * chan], proj[2 * chan:]
        v_t[c, :, pl.ds(lo, width)] = v[:, :width].astype(BF16)
        gate_t[c, :, pl.ds(lo, LANES)] = jax.nn.sigmoid(gl)
        if lo == 0:
            qmask[c, :, pl.ds(0, LANES)] = q.astype(BF16)
        else:
            for h in range(heads):
                keep = low if h % 2 == 0 else jnp.logical_not(low)
                qmask[c, pl.ds(h * dim, dim), pl.ds(LANES, LANES)] = jnp.where(keep, q[h * dim:(h + 1) * dim], 0.0).astype(BF16)

    def end_first(i):
        wb = w_b[...].astype(BF16)
        u = jnp.concatenate([layer_norm(flat[pl.ds(2 * i + j, LANES, stride=rows), :]) for j in range(2)], axis=0)
        b = mm(wb, u, ((1,), (1,)))
        k = mm(u, wqe_ref[:, pl.ds(chan, chan)]).astype(BF16)
        proj = mm(w_t[...], u, ((1,), (1,)))
        for j in range(2):
            cut = slice(j * LANES, (j + 1) * LANES)
            put_bias(2 * i + j, 0, b[:, cut], None)
            keys[2 * i + j, pl.ds(0, LANES)] = k[cut]
            put_projected(2 * i + j, proj[:, cut], 0, LANES)

    def end_second(i):
        wb = w_b[...].astype(BF16)
        u = [layer_norm(flat[pl.ds(LANES * rows + 2 * i + j, tail, stride=rows), :]) for j in range(2)]
        u = jnp.concatenate([u[0], u[0], u[1], u[1]], axis=0)
        norm_b[i] = u
        b = mm(wb, u, ((1,), (1,)))
        for j in range(2):
            cut = slice(j * LANES, (j + 1) * LANES)
            put_bias(2 * i + j, 1, b[:, cut], b[:, cut])

    def end_third(i):
        u = norm_b[i]
        k = mm(jnp.concatenate([u[:tail], u[LANES:LANES + tail]], axis=0), wqe_ref[:, pl.ds(chan, chan)]).astype(BF16)
        proj = mm(w_t[...], u, ((1,), (1,)))
        for j in range(2):
            keys[2 * i + j, pl.ds(LANES, tail)] = k[j * tail:(j + 1) * tail]
            put_projected(2 * i + j, proj[:, j * LANES:(j + 1) * LANES], LANES, tail)

    def start_project(r):
        u = norm[r]
        keys[r] = mm(u, wqs_ref[:, pl.ds(chan, chan)]).astype(BF16)
        proj = mm(w_t[...], doubled(u), ((1,), (1,)))
        put_projected(r, proj[:, :LANES], 0, LANES)
        put_projected(r, proj[:, LANES:], LANES, tail)

    def spread_bias(phase):
        wait_recv(bias_in.at[phase, others], bias_sem.at[phase])
        for pair in range(heads // 2):
            tiles = []
            for t in range(3):
                b = bias_in[phase, :, pair, t].astype(F32)
                if phase == 0:
                    b = doubled(b.reshape(seq, LANES))
                else:
                    late = b[:, early // 8:].reshape(tail, LANES)
                    b = jnp.concatenate([b[:, :early // 8].reshape(LANES, LANES), late, late], axis=0)
                tiles.append(b.T)
            t0, t1, t2 = tiles
            even = jnp.concatenate([t0, t2[:tail]], axis=0)
            odd = jnp.concatenate([t1, t2[tail:]], axis=0)
            bias_t[pair, :, pl.ds(0, LANES)] = even[:, :LANES]
            bias_t[pair, :, pl.ds(LANES, LANES)] = odd[:, :LANES]
            bias_t[2, :, pl.ds(pair * LANES, LANES)] = jnp.where(low, even[:, LANES:], odd[:, LANES:])

    zero = jnp.zeros((dim, LANES), BF16)
    zero2 = jnp.zeros((2 * dim, LANES), BF16)
    zero4 = jnp.zeros((2 * dim, 2 * LANES), BF16)

    def query_tile(r, t):
        if t == 2:
            top = jnp.concatenate([qmask[r, pl.ds(0, 2 * dim), pl.ds(LANES, LANES)], zero2], axis=1)
            bottom = jnp.concatenate([zero2, qmask[r, pl.ds(2 * dim, 2 * dim), pl.ds(LANES, LANES)]], axis=1)
            return jnp.concatenate([top, bottom], axis=0)
        first = qmask[r, pl.ds(2 * t * dim, dim), pl.ds(0, LANES)]
        second = qmask[r, pl.ds((2 * t + 1) * dim, dim), pl.ds(0, LANES)]
        pair = jnp.concatenate([jnp.concatenate([first, zero], axis=1), jnp.concatenate([zero, second], axis=1)], axis=0)
        return jnp.concatenate([pair, zero4] if t == 0 else [zero4, pair], axis=0)

    def score_tile(r, t):
        s = mm(keys[r], query_tile(r, t)) * scale + bias_t[t]
        scores[t] = s
        tops[t] = jnp.max(s, axis=0, keepdims=True)

    def mix_tile(r, t):
        e = jnp.exp(scores[t] - tops[t])
        total = jnp.sum(e, axis=0, keepdims=True)
        values = v_t[r] if t == 2 else v_t[r, pl.ds(2 * t * dim, 2 * dim), :]
        o = mm(values, e.astype(BF16)) * (1.0 / total)
        if t < 2:
            for h in (2 * t, 2 * t + 1):
                part = o[(h % 2) * dim:(h % 2 + 1) * dim, (h % 2) * LANES:(h % 2 + 1) * LANES]
                mixed[pl.ds(h * dim, dim), pl.ds(0, LANES)] = (part * gate_t[r, pl.ds(h * dim, dim), pl.ds(0, LANES)]).astype(BF16)
        else:
            for h in range(heads):
                part = o[h * dim:(h + 1) * dim, (h // 2) * LANES:(h // 2 + 1) * LANES] * gate_t[r, pl.ds(h * dim, dim), pl.ds(LANES, LANES)]
                mixed[pl.ds(h * dim, dim), pl.ds(LANES, LANES)] = jnp.where(low if h % 2 == 0 else jnp.logical_not(low), part, 0.0).astype(BF16)

    def merge_heads(wo):
        upd = mm(mixed[...].T, wo)
        return jnp.concatenate([upd[:LANES], upd[LANES:LANES + tail] + upd[LANES + tail:]], axis=0)

    def pipeline(steps, lag):
        def step(idx, carry):
            steps(idx, lambda back: jnp.clip(idx - back, 0, rows - 1))
            return carry

        lax.fori_loop(0, rows + lag, step, 0)

    def send_rows(last, src, dst, sem):
        @pl.when(jnp.logical_and(last >= 0, lax.rem(last, SEND) == SEND - 1))
        def _():
            first = last - (SEND - 1)
            some = pl.ds(first, SEND)
            dst[me, some] = src[some, pl.ds(me * sub, sub)]
            peers(lambda d: remote(src.at[some, pl.ds(d * sub, sub)], dst.at[me, some], sem(first), d).start())

    def unpack(src, lo, count, base):
        def part(d):
            flat[pl.ds(base + d * count * rows, count * rows), :] = src[d, pl.ds(lo, count)].astype(F32).reshape(count * rows, chan)

        loop(group, part)

    loads[0].wait()
    loads[1].wait()
    load_weights(wqs_ref, wbs_ref)
    start_norm()
    loop(rows, start_project, 2)
    for load in loads[2:]:
        load.wait()
    spread_bias(0)

    def start_step(idx, at):
        r = at(2)
        z_new = z_ref[r] + merge_heads(wos_ref[...])
        out_ref[r] = z_new
        h_out[r] = z_new.astype(BF16).reshape(seq // 8, 8, chan)
        for t in range(3):
            mix_tile(at(1), t)
            score_tile(at(0), t)
        send_rows(idx - 2, h_out, h_in, lambda first: h_sem.at[first // early])

    pipeline(start_step, 2)

    load_weights(wqe_ref, wbe_ref)
    wait_recv(h_in.at[others, pl.ds(0, early)], h_sem.at[0])
    unpack(h_in, 0, early, 0)
    loop(rows // 2, end_first)
    send_bias(1, pl.ds(0, 2), pl.ds(0, rows))
    wait_recv(h_in.at[others, pl.ds(early, rows - early)], h_sem.at[1])
    unpack(h_in, early, rows - early, LANES * rows)
    loop(rows // 2, end_second, 2)
    send_bias(1, pl.ds(2, 1), pl.ds(0, rows))
    loop(rows // 2, end_third)
    spread_bias(1)
    column = lambda c: flat[pl.ds(c, seq, stride=rows), :]

    def by_owner(vals):
        parts = vals.reshape(seq // 8, 8, chan)
        base = LANES // 8
        order = []
        for d in range(group):
            order.append(parts[d * early // 8:(d + 1) * early // 8])
            order.append(parts[base + d * (sub - early // 8):base + (d + 1) * (sub - early // 8)])
        return jnp.concatenate(order, axis=0)

    def end_step(idx, at):
        hidden = jnp.maximum(mm(normed[...], w1_ref[...]), 0.0).astype(BF16)
        d_out[at(3)] = by_owner(upds[...] + mm(hidden, w2_ref[...])).astype(BF16)
        upd = merge_heads(woe_ref[...])
        upds[...] = upd
        normed[...] = layer_norm(column(at(2)) + upd)
        for t in range(3):
            mix_tile(at(1), t)
            score_tile(at(0), t)
        send_rows(idx - 3, d_out, d_in, lambda first: d_sem)

    pipeline(end_step, 3)
    wait_recv(d_in.at[others], d_sem)
    unpack(d_in, 0, rows, 0)

    def final(r):
        out_ref[r] = out_ref[r] + flat[pl.ds(r, seq, stride=rows), :]

    loop(rows, final, 2)
    for phase in range(2):
        wait_send(bias_in.at[phase, others])
    wait_send(h_in.at[others])
    wait_send(d_in.at[others])


def solution(mesh):
    axis = 'sp'
    group = mesh.shape[axis]
    row_spec = P(('dp', 'sp'), None, None)

    def local_fn(pair_loc, w_qkvg_s, w_bias_s, w_out_s, w_qkvg_e, w_bias_e, w_out_e, w_one, w_two):
        rows, seq, chan = pair_loc.shape
        heads = w_bias_s.shape[0]
        sub = rows // 8
        packed = 2 * LANES
        weights = (w_qkvg_s, w_bias_s, w_out_s, w_qkvg_e, w_bias_e, w_out_e, w_one, w_two)
        scratch = [pltpu.VMEM(pair_loc.shape, F32)] + [pltpu.VMEM(w.shape, w.dtype) for w in weights] + [
            pltpu.VMEM((rows * seq, chan), F32),
            pltpu.VMEM((rows, seq, chan), BF16),
            pltpu.VMEM((rows // 2, packed, chan), BF16),
            pltpu.VMEM((3 * chan, chan), BF16),
            pltpu.VMEM((16, chan), F32),
            pltpu.VMEM((rows, chan, packed), BF16),
            pltpu.VMEM((rows, chan, seq), BF16),
            pltpu.VMEM((rows, chan, packed), F32),
            pltpu.VMEM((rows, seq, chan), BF16),
            pltpu.VMEM((heads // 2, 3, rows, LANES), F32),
            pltpu.VMEM((2, heads // 2, 3, sub, 8, LANES), BF16),
            pltpu.VMEM((2, group, heads // 2, 3, sub, 8, LANES), BF16),
            pltpu.VMEM((3, seq, packed), F32),
            pltpu.VMEM((3, seq, packed), F32),
            pltpu.VMEM((3, 1, packed), F32),
            pltpu.VMEM((chan, packed), BF16),
            pltpu.VMEM((seq, chan), F32),
            pltpu.VMEM((seq, chan), BF16),
            pltpu.VMEM((rows, seq // 8, 8, chan), BF16),
            pltpu.VMEM((group, rows, sub, 8, chan), BF16),
            pltpu.VMEM((rows, seq // 8, 8, chan), BF16),
            pltpu.VMEM((group, rows, sub, 8, chan), BF16),
            pltpu.SemaphoreType.DMA((sub,)),
            pltpu.SemaphoreType.DMA((len(weights),)),
            pltpu.SemaphoreType.DMA,
            pltpu.SemaphoreType.DMA((2,)),
            pltpu.SemaphoreType.DMA((2,)),
            pltpu.SemaphoreType.DMA,
        ]
        return pl.pallas_call(
            functools.partial(kernel, (group, rows, seq, chan, heads, axis)),
            out_shape=jax.ShapeDtypeStruct(pair_loc.shape, F32),
            in_specs=[pl.BlockSpec(memory_space=pltpu.HBM)] * 9,
            out_specs=pl.BlockSpec(memory_space=pltpu.VMEM),
            scratch_shapes=scratch,
            compiler_params=pltpu.CompilerParams(collective_id=0, has_side_effects=True, vmem_limit_bytes=40 * 2 ** 20),
        )(*[pltpu.with_memory_space_constraint(x, pltpu.HBM) for x in (pair_loc, *weights)])

    return jax.shard_map(local_fn, mesh=mesh, in_specs=(row_spec, P(), P(), P(), P(), P(), P(), P(), P()), out_specs=row_spec, check_vma=False)
```

```python
import functools

import jax
import jax.numpy as jnp
from jax import lax
from jax.experimental import pallas as pl
from jax.experimental.pallas import tpu as pltpu
from jax.sharding import PartitionSpec as P

LN_EPS = 1e-5
LANES = 128
SEND = 2
F32, BF16 = jnp.float32, jnp.bfloat16


def layer_norm(vals):
    mean = jnp.mean(vals, axis=-1, keepdims=True)
    centered = vals - mean
    var = jnp.mean(centered * centered, axis=-1, keepdims=True)
    return (centered * lax.rsqrt(var + LN_EPS)).astype(BF16)


def mm(lhs, rhs, contract=((1,), (0,))):
    return lax.dot_general(lhs, rhs, (contract, ((), ())), preferred_element_type=F32)


def loop(count, body, unroll=1):
    def step(idx, carry):
        for sub in range(unroll):
            body(idx * unroll + sub)
        return carry

    lax.fori_loop(0, count // unroll, step, 0)


def kernel(cfg, z_hbm, wqs_hbm, wbs_hbm, wos_hbm, wqe_hbm, wbe_hbm, woe_hbm, w1_hbm, w2_hbm, out_ref,
           z_ref, wqs_ref, wbs_ref, wos_ref, wqe_ref, wbe_ref, woe_ref, w1_ref, w2_ref,
           flat, norm, w_b, qmask, v_t, gate, keys, bias_rows, bias_out, bias_in, bias_t, scores, tops, mixed, upds, normed,
           h_out, h_in, d_out, d_in, z_sem, w_sem, out_sem, start_sem, far_sem, near_sem, h_sem, d_sem):
    group, rows, seq, chan, heads, axis = cfg
    dim = chan // heads
    me = lax.axis_index(axis)
    tail = seq - LANES
    sub = rows // 8
    scale = dim ** -0.5
    early = LANES // group

    loads = []
    pairs = ((wqs_hbm, wqs_ref), (wbs_hbm, wbs_ref), (wos_hbm, wos_ref), (wqe_hbm, wqe_ref),
             (wbe_hbm, wbe_ref), (woe_hbm, woe_ref), (w1_hbm, w1_ref), (w2_hbm, w2_ref))
    z_copy = lambda g: pltpu.make_async_copy(z_hbm.at[pl.ds(g * 8, 8)], z_ref.at[pl.ds(g * 8, 8)], z_sem.at[g])
    for g in range(sub):
        z_copy(g).start()
    for i, (src, dst) in enumerate(pairs):
        loads.append(pltpu.make_async_copy(src, dst, w_sem.at[i]))
        loads[i].start()

    barrier = pltpu.get_barrier_semaphore()
    for off in range(1, group):
        pl.semaphore_signal(barrier, inc=1, device_id={axis: lax.rem(me + off, group)}, device_id_type=pl.DeviceIdType.MESH)

    lane = lax.broadcasted_iota(jnp.int32, (1, LANES), 1)
    low = lane < tail
    even_head = (lane // dim) % 2 == 0

    def doubled(rows_in):
        return jnp.concatenate([rows_in, rows_in[LANES:seq]], axis=0)

    def peers(start):
        for off in range(1, group):
            start(lax.rem(me + off, group))

    def remote(src, dst, recv, dst_dev):
        return pltpu.make_async_remote_copy(src_ref=src, dst_ref=dst, send_sem=out_sem, recv_sem=recv,
                                            device_id={axis: dst_dev}, device_id_type=pl.DeviceIdType.MESH)

    def wait_recv(part, sem):
        pltpu.make_async_remote_copy(src_ref=part, dst_ref=part, send_sem=out_sem, recv_sem=sem,
                                     device_id={axis: me}, device_id_type=pl.DeviceIdType.MESH).wait_recv()

    def wait_send(part):
        pltpu.make_async_remote_copy(src_ref=part, dst_ref=part, send_sem=out_sem, recv_sem=out_sem,
                                     device_id={axis: me}, device_id_type=pl.DeviceIdType.MESH).wait_send()

    others = pl.ds(0, group - 1)

    def load_bias_weight(phase, wb_ref):
        w_b[phase] = jnp.zeros(w_b.shape[1:], w_b.dtype)
        w_b[phase, pl.ds(0, heads), :] = wb_ref[...].astype(F32)

    def put_bias(r, wb, u):
        b = mm(wb, doubled(u), ((1,), (1,)))
        for pair in range(heads // 2):
            even, odd = b[2 * pair:2 * pair + 1], b[2 * pair + 1:2 * pair + 2]
            bias_rows[pair, 0, pl.ds(r, 1), :] = even[:, :LANES]
            bias_rows[pair, 1, pl.ds(r, 1), :] = odd[:, :LANES]
            bias_rows[pair, 2, pl.ds(r, 1), :] = jnp.where(low, even[:, LANES:], odd[:, LANES:])

    def round_bias(phase, g):
        rounded = bias_rows[:, :, pl.ds(pl.multiple_of(g * 8, 8), 8)].astype(BF16).reshape(heads // 2, 3, 1, 8, LANES)
        bias_out[phase, :, :, pl.ds(g, 1)] = rounded
        bias_in[phase, me, :, :, pl.ds(g, 1)] = rounded

    def bias_copy(phase, g, src, slot, sem, d):
        return remote(src, bias_in.at[phase, slot, :, :, pl.ds(g, 1)], sem, d)

    def send_start_bias(g):
        round_bias(0, g)
        src = bias_out.at[0, :, :, pl.ds(g, 1)]
        peers(lambda d: bias_copy(0, g, src, me, start_sem, d).start())

    twin = me + 1 - 2 * lax.rem(me, 2)

    def send_end_bias(g):
        round_bias(1, g)
        src = bias_out.at[1, :, :, pl.ds(g, 1)]
        for off in range(2, group, 2):
            bias_copy(1, g, src, me, far_sem.at[g], lax.rem(me + off, group)).start()
        bias_copy(1, g, src, me, near_sem, twin).start()

    def relay_bias(g):
        wait_recv(bias_in.at[1, pl.ds(0, group // 2 - 1), :, :, pl.ds(g, 1)], far_sem.at[g])
        for off in range(2, group, 2):
            slot = lax.rem(me + off, group)
            bias_copy(1, g, bias_in.at[1, slot, :, :, pl.ds(g, 1)], slot, near_sem, twin).start()

    def start_norm():
        wb = w_b[0].astype(BF16)
        for g in range(sub):
            z_copy(g).wait()

            def row(i):
                r = g * 8 + i
                u = layer_norm(z_ref[r])
                norm[r] = u
                put_bias(r, wb, u)

            loop(8, row, 4)
            if g == 0:
                pl.semaphore_wait(barrier, group - 1)
            send_start_bias(g)

    def project(c, u, lo, width, wq):
        y = mm(u, wq)
        q, k, v, gl = [y[:, i * chan:(i + 1) * chan] for i in range(4)]
        keys[c, pl.ds(lo, width)] = k.astype(BF16)
        gate[c, pl.ds(lo, width)] = jax.nn.sigmoid(gl)
        late = q[width - tail:]
        masked = [jnp.where(even_head, late, 0.0), jnp.where(even_head, 0.0, late)]
        twice = [v[width - tail:], v[width - tail:]]
        if lo == 0:
            qmask[c, :, pl.ds(0, LANES)] = q[:LANES].astype(BF16).T
            v_t[c, :, pl.ds(0, LANES)] = v[:LANES].astype(BF16).T
        if lo + width == seq:
            qmask[c, :, pl.ds(LANES, LANES)] = jnp.concatenate(masked, axis=0).astype(BF16).T
            v_t[c, :, pl.ds(LANES, LANES)] = jnp.concatenate(twice, axis=0).astype(BF16).T

    def spread_start_bias():
        wait_recv(bias_in.at[0, others], start_sem)
        for pair in range(heads // 2):
            t0, t1, t2 = [doubled(bias_in[0, :, pair, t].astype(F32).reshape(seq, LANES)).T for t in range(3)]
            even = jnp.concatenate([t0, t2[:tail]], axis=0)
            odd = jnp.concatenate([t1, t2[tail:]], axis=0)
            bias_t[pair, :, pl.ds(0, LANES)] = even[:, :LANES]
            bias_t[pair, :, pl.ds(LANES, LANES)] = odd[:, :LANES]
            bias_t[2, :, pl.ds(pair * LANES, LANES)] = jnp.where(low, even[:, LANES:], odd[:, LANES:])

    def spread_end_bias():
        wait_recv(bias_in.at[1, pl.ds(0, group // 2)], near_sem)
        for pair in range(heads // 2):
            for t in range(3):
                b = bias_in[1, :, pair, t].astype(F32)
                b = jnp.concatenate([b[:, :early // 8].reshape(LANES, LANES), b[:, early // 8:].reshape(tail, LANES)], axis=0)
                if t < 2:
                    bias_t[pair, :, pl.ds(t * LANES, LANES)] = b
                else:
                    bias_t[2, :, pl.ds(pair * LANES, LANES)] = b

    zero = jnp.zeros((dim, LANES), BF16)
    zero2 = jnp.zeros((2 * dim, LANES), BF16)
    zero4 = jnp.zeros((2 * dim, 2 * LANES), BF16)

    def query_tile(r, t):
        if t == 2:
            top = jnp.concatenate([qmask[r, pl.ds(0, 2 * dim), pl.ds(LANES, LANES)], zero2], axis=1)
            bottom = jnp.concatenate([zero2, qmask[r, pl.ds(2 * dim, 2 * dim), pl.ds(LANES, LANES)]], axis=1)
            return jnp.concatenate([top, bottom], axis=0)
        first = qmask[r, pl.ds(2 * t * dim, dim), pl.ds(0, LANES)]
        second = qmask[r, pl.ds((2 * t + 1) * dim, dim), pl.ds(0, LANES)]
        pair = jnp.concatenate([jnp.concatenate([first, zero], axis=1), jnp.concatenate([zero, second], axis=1)], axis=0)
        return jnp.concatenate([pair, zero4] if t == 0 else [zero4, pair], axis=0)

    def score_tile(r, slot, t):
        s = mm(keys[r], query_tile(r, t)) * scale + bias_t[t]
        scores[slot, t] = s
        tops[slot, t] = jnp.max(s, axis=0, keepdims=True)

    def mix_tile(r, slot, t):
        e = jnp.exp(scores[slot, t] - tops[slot, t])
        total = jnp.sum(e, axis=0, keepdims=True)
        values = v_t[r, :, pl.ds(0, seq)] if t == 2 else v_t[r, pl.ds(2 * t * dim, 2 * dim), pl.ds(0, seq)]
        o = mm(values, e.astype(BF16)) * (1.0 / total)
        if t < 2:
            for h in (2 * t, 2 * t + 1):
                mixed[slot, pl.ds(h * dim, dim), pl.ds(0, LANES)] = o[(h % 2) * dim:(h % 2 + 1) * dim, (h % 2) * LANES:(h % 2 + 1) * LANES]
        else:
            for h in range(heads):
                mixed[slot, pl.ds(h * dim, dim), pl.ds(LANES, LANES)] = o[h * dim:(h + 1) * dim, (h // 2) * LANES:(h // 2 + 1) * LANES]

    def merge_heads(r, slot, wo):
        o = mixed[slot].T
        o = jnp.concatenate([o[:LANES], jnp.where(even_head, o[LANES:LANES + tail], o[LANES + tail:])], axis=0)
        return mm((o * gate[r]).astype(BF16), wo)

    def pipeline(stages, send):
        depth, count = len(stages), rows // 2

        def turn(i, active):
            for stage in sorted(active, reverse=True):
                for slot in range(2):
                    stages[stage](2 * (i - stage) + slot, slot)
            send(i, active)

        for i in range(depth - 1):
            turn(i, range(i + 1))

        def step(i, carry):
            turn(i, range(depth))
            return carry

        lax.fori_loop(depth - 1, count, step, 0)
        for i in range(count, count + depth - 1):
            turn(i, range(i - count + 1, depth))

    def score(r, slot):
        for t in range(3):
            score_tile(r, slot, t)

    def mix(r, slot):
        for t in range(3):
            mix_tile(r, slot, t)

    def send_rows(first, src, dst, sem):
        some = pl.ds(first, SEND)
        dst[me, some] = src[some, pl.ds(me * sub, sub)]
        peers(lambda d: remote(src.at[some, pl.ds(d * sub, sub)], dst.at[me, some], sem(first), d).start())

    def unpack(src, lo, count, base):
        def part(d):
            flat[pl.ds(base + d * count * rows, count * rows), :] = src[d, pl.ds(lo, count)].astype(F32).reshape(count * rows, chan)

        loop(group, part)

    def by_place(vals):
        parts = vals.reshape(group, sub, 8, chan)
        return jnp.concatenate([parts[:, :early // 8].reshape(LANES, chan), parts[:, early // 8:].reshape(tail, chan)], axis=0)

    loads[1].wait()
    load_bias_weight(0, wbs_ref)
    start_norm()
    loads[0].wait()
    loop(rows, lambda r: project(r, norm[r], 0, seq, wqs_ref[...]), 2)
    for load in loads[2:]:
        load.wait()
    load_bias_weight(1, wbe_ref)
    spread_start_bias()

    def start_merge(r, slot):
        z_new = z_ref[r] + merge_heads(r, slot, wos_ref[...])
        out_ref[r] = z_new
        h_out[r] = z_new.astype(BF16).reshape(seq // 8, 8, chan)

    def end_bias(r, slot):
        h = out_ref[r].astype(BF16).astype(F32)
        put_bias(r, w_b[1].astype(BF16), layer_norm(by_place(h)))

    def start_send(i, active):
        if 2 in active:
            send_rows(2 * (i - 2), h_out, h_in, lambda r: h_sem.at[r // early])
        if 3 in active:
            r = 2 * (i - 3)
            if isinstance(r, int):
                if r % 8 == 6:
                    send_end_bias(r // 8)
            else:
                @pl.when(lax.rem(r, 8) == 6)
                def _():
                    send_end_bias(r // 8)

    pipeline((score, mix, start_merge, end_bias), start_send)

    for g in range(sub - 1):
        relay_bias(g)
    wait_recv(h_in.at[others, pl.ds(0, early)], h_sem.at[0])
    unpack(h_in, 0, early, 0)

    def end_project(lo, width):
        return lambda c: project(c, layer_norm(flat[pl.ds(lo * rows + c, width, stride=rows), :]), lo, width, wqe_ref[...])

    loop(rows, end_project(0, LANES), 2)
    wait_recv(h_in.at[others, pl.ds(early, rows - early)], h_sem.at[1])
    relay_bias(sub - 1)
    unpack(h_in, early, rows - early, LANES * rows)
    loop(rows, end_project(LANES, tail), 4)
    spread_end_bias()
    column = lambda c: flat[pl.ds(c, seq, stride=rows), :]

    def by_owner(vals):
        parts = vals.reshape(seq // 8, 8, chan)
        base = LANES // 8
        order = []
        for d in range(group):
            order.append(parts[d * early // 8:(d + 1) * early // 8])
            order.append(parts[base + d * (sub - early // 8):base + (d + 1) * (sub - early // 8)])
        return jnp.concatenate(order, axis=0)

    def end_merge(c, slot):
        upd = merge_heads(c, slot, woe_ref[...])
        upds[slot] = upd
        normed[slot] = layer_norm(column(c) + upd)

    def transition(c, slot):
        hidden = jnp.maximum(mm(normed[slot], w1_ref[...]), 0.0).astype(BF16)
        d_out[c] = by_owner(upds[slot] + mm(hidden, w2_ref[...])).astype(BF16)

    def end_send(i, active):
        if 3 in active:
            send_rows(2 * (i - 3), d_out, d_in, lambda c: d_sem.at[c // 8])

    pipeline((score, mix, end_merge, transition), end_send)
    for g in range(sub):
        wait_recv(d_in.at[others, pl.ds(g * 8, 8)], d_sem.at[g])

        def part(d):
            flat[pl.ds((d * rows + g * 8) * rows, 8 * rows), :] = d_in[d, pl.ds(g * 8, 8)].astype(F32).reshape(8 * rows, chan)

        loop(group, part, 2)

        def final(r):
            for d in range(group):
                at = d * rows + g * 8
                out_ref[r, pl.ds(at, 8), :] = out_ref[r, pl.ds(at, 8), :] + flat[pl.ds(at * rows + r, 8, stride=rows), :]

        loop(rows, final, 4)

    for phase in range(2):
        wait_send(bias_in.at[phase, others])
    wait_send(h_in.at[others])
    wait_send(d_in.at[others])


def solution(mesh):
    axis = 'sp'
    group = mesh.shape[axis]
    row_spec = P(('dp', 'sp'), None, None)

    def local_fn(pair_loc, w_qkvg_s, w_bias_s, w_out_s, w_qkvg_e, w_bias_e, w_out_e, w_one, w_two):
        rows, seq, chan = pair_loc.shape
        heads = w_bias_s.shape[0]
        sub = rows // 8
        packed = 2 * LANES
        weights = (w_qkvg_s, w_bias_s, w_out_s, w_qkvg_e, w_bias_e, w_out_e, w_one, w_two)
        scratch = [pltpu.VMEM(pair_loc.shape, F32)] + [pltpu.VMEM(w.shape, w.dtype) for w in weights] + [
            pltpu.VMEM((rows * seq, chan), F32),
            pltpu.VMEM((rows, seq, chan), BF16),
            pltpu.VMEM((2, 16, chan), F32),
            pltpu.VMEM((rows, chan, packed), BF16),
            pltpu.VMEM((rows, chan, packed), BF16),
            pltpu.VMEM((rows, seq, chan), F32),
            pltpu.VMEM((rows, seq, chan), BF16),
            pltpu.VMEM((heads // 2, 3, rows, LANES), F32),
            pltpu.VMEM((2, heads // 2, 3, sub, 8, LANES), BF16),
            pltpu.VMEM((2, group, heads // 2, 3, sub, 8, LANES), BF16),
            pltpu.VMEM((3, seq, packed), F32),
            pltpu.VMEM((2, 3, seq, packed), F32),
            pltpu.VMEM((2, 3, 1, packed), F32),
            pltpu.VMEM((2, chan, packed), F32),
            pltpu.VMEM((2, seq, chan), F32),
            pltpu.VMEM((2, seq, chan), BF16),
            pltpu.VMEM((rows, seq // 8, 8, chan), BF16),
            pltpu.VMEM((group, rows, sub, 8, chan), BF16),
            pltpu.VMEM((rows, seq // 8, 8, chan), BF16),
            pltpu.VMEM((group, rows, sub, 8, chan), BF16),
            pltpu.SemaphoreType.DMA((sub,)),
            pltpu.SemaphoreType.DMA((len(weights),)),
            pltpu.SemaphoreType.DMA,
            pltpu.SemaphoreType.DMA,
            pltpu.SemaphoreType.DMA((sub,)),
            pltpu.SemaphoreType.DMA,
            pltpu.SemaphoreType.DMA((2,)),
            pltpu.SemaphoreType.DMA((sub,)),
        ]
        return pl.pallas_call(
            functools.partial(kernel, (group, rows, seq, chan, heads, axis)),
            out_shape=jax.ShapeDtypeStruct(pair_loc.shape, F32),
            in_specs=[pl.BlockSpec(memory_space=pltpu.HBM)] * 9,
            out_specs=pl.BlockSpec(memory_space=pltpu.VMEM),
            scratch_shapes=scratch,
            compiler_params=pltpu.CompilerParams(collective_id=0, has_side_effects=True, vmem_limit_bytes=40 * 2 ** 20),
        )(*[pltpu.with_memory_space_constraint(x, pltpu.HBM) for x in (pair_loc, *weights)])

    return jax.shard_map(local_fn, mesh=mesh, in_specs=(row_spec, P(), P(), P(), P(), P(), P(), P(), P()), out_specs=row_spec, check_vma=False)
```

```python
import functools

import jax
import jax.numpy as jnp
from jax import lax
from jax.experimental import pallas as pl
from jax.experimental.pallas import tpu as pltpu
from jax.sharding import PartitionSpec as P

LN_EPS = 1e-5
LANES = 128
SEND = 2
F32, BF16 = jnp.float32, jnp.bfloat16


def layer_norm(vals):
    mean = jnp.mean(vals, axis=-1, keepdims=True)
    centered = vals - mean
    var = jnp.mean(centered * centered, axis=-1, keepdims=True)
    return (centered * lax.rsqrt(var + LN_EPS)).astype(BF16)


def mm(lhs, rhs, contract=((1,), (0,))):
    return lax.dot_general(lhs, rhs, (contract, ((), ())), preferred_element_type=F32)


def loop(count, body, unroll=1):
    def step(idx, carry):
        for sub in range(unroll):
            body(idx * unroll + sub)
        return carry

    lax.fori_loop(0, count // unroll, step, 0)


def kernel(cfg, z_hbm, wqs_hbm, wbs_hbm, wos_hbm, wqe_hbm, wbe_hbm, woe_hbm, w1_hbm, w2_hbm, out_ref,
           z_ref, wqs_ref, wbs_ref, wos_ref, wqe_ref, wbe_ref, woe_ref, w1_ref, w2_ref,
           flat, norm, w_b, qmask, v_t, gate, keys, bias_rows, bias_out, bias_in, bias_t, scores, tops, mixed, upds, normed,
           h_out, h_in, d_out, d_in, z_sem, w_sem, out_sem, far_sem, near_sem, h_sem, d_sem):
    group, rows, seq, chan, heads, axis = cfg
    dim = chan // heads
    me = lax.axis_index(axis)
    tail = seq - LANES
    sub = rows // 8
    scale = dim ** -0.5
    early = LANES // group

    loads = []
    pairs = ((wqs_hbm, wqs_ref), (wbs_hbm, wbs_ref), (wos_hbm, wos_ref), (wqe_hbm, wqe_ref),
             (wbe_hbm, wbe_ref), (woe_hbm, woe_ref), (w1_hbm, w1_ref), (w2_hbm, w2_ref))
    z_copy = lambda g: pltpu.make_async_copy(z_hbm.at[pl.ds(g * 8, 8)], z_ref.at[pl.ds(g * 8, 8)], z_sem.at[g])
    for g in range(sub):
        z_copy(g).start()
    for i, (src, dst) in enumerate(pairs):
        loads.append(pltpu.make_async_copy(src, dst, w_sem.at[i]))
    loads[1].start()

    barrier = pltpu.get_barrier_semaphore()
    for off in range(1, group):
        pl.semaphore_signal(barrier, inc=1, device_id={axis: lax.rem(me + off, group)}, device_id_type=pl.DeviceIdType.MESH)

    lane = lax.broadcasted_iota(jnp.int32, (1, LANES), 1)
    low = lane < tail
    even_head = (lane // dim) % 2 == 0

    def doubled(rows_in):
        return jnp.concatenate([rows_in, rows_in[LANES:seq]], axis=0)

    def peers(start):
        for off in range(1, group):
            start(lax.rem(me + off, group))

    def remote(src, dst, recv, dst_dev):
        return pltpu.make_async_remote_copy(src_ref=src, dst_ref=dst, send_sem=out_sem, recv_sem=recv,
                                            device_id={axis: dst_dev}, device_id_type=pl.DeviceIdType.MESH)

    def wait_recv(part, sem):
        pltpu.make_async_remote_copy(src_ref=part, dst_ref=part, send_sem=out_sem, recv_sem=sem,
                                     device_id={axis: me}, device_id_type=pl.DeviceIdType.MESH).wait_recv()

    def wait_send(part):
        pltpu.make_async_remote_copy(src_ref=part, dst_ref=part, send_sem=out_sem, recv_sem=out_sem,
                                     device_id={axis: me}, device_id_type=pl.DeviceIdType.MESH).wait_send()

    others = pl.ds(0, group - 1)

    def load_bias_weight(phase, wb_ref):
        w_b[phase] = jnp.zeros(w_b.shape[1:], w_b.dtype)
        w_b[phase, pl.ds(0, heads), :] = wb_ref[...].astype(F32)

    def put_bias(r, wb, u):
        b = mm(wb, doubled(u), ((1,), (1,)))
        for pair in range(heads // 2):
            even, odd = b[2 * pair:2 * pair + 1], b[2 * pair + 1:2 * pair + 2]
            bias_rows[pair, 0, pl.ds(r, 1), :] = even[:, :LANES]
            bias_rows[pair, 1, pl.ds(r, 1), :] = odd[:, :LANES]
            bias_rows[pair, 2, pl.ds(r, 1), :] = jnp.where(low, even[:, LANES:], odd[:, LANES:])

    def round_bias(phase, g):
        rounded = bias_rows[:, :, pl.ds(pl.multiple_of(g * 8, 8), 8)].astype(BF16).reshape(heads // 2, 3, 1, 8, LANES)
        bias_out[phase, :, :, pl.ds(g, 1)] = rounded
        bias_in[phase, me, :, :, pl.ds(g, 1)] = rounded

    twin = me + 1 - 2 * lax.rem(me, 2)

    def bias_copy(phase, g, src, slot, sem, d):
        remote(src, bias_in.at[phase, slot, :, :, pl.ds(g, 1)], sem.at[phase, g], d).start()

    def send_bias(phase, g, direct):
        round_bias(phase, g)
        src = bias_out.at[phase, :, :, pl.ds(g, 1)]
        for off in range(1, group):
            if off % 2 == 0:
                bias_copy(phase, g, src, me, far_sem, lax.rem(me + off, group))
            elif direct:
                bias_copy(phase, g, src, me, near_sem, lax.rem(me + off, group))
        if not direct:
            bias_copy(phase, g, src, me, near_sem, twin)

    def await_bias(phase, g, direct):
        wait_recv(bias_in.at[phase, pl.ds(0, group // 2 - 1), :, :, pl.ds(g, 1)], far_sem.at[phase, g])
        if not direct:
            for off in range(2, group, 2):
                slot = lax.rem(me + off, group)
                bias_copy(phase, g, bias_in.at[phase, slot, :, :, pl.ds(g, 1)], slot, near_sem, twin)

    def await_twin(phase, g):
        wait_recv(bias_in.at[phase, pl.ds(0, group // 2), :, :, pl.ds(g, 1)], near_sem.at[phase, g])

    def start_norm():
        wb = w_b[0].astype(BF16)
        for g in range(sub):
            z_copy(g).wait()

            def row(i):
                r = g * 8 + i
                u = layer_norm(z_ref[r])
                norm[r] = u
                put_bias(r, wb, u)

            loop(8, row, 4)
            if g == 0:
                for i, load in enumerate(loads):
                    if i != 1:
                        load.start()
                pl.semaphore_wait(barrier, group - 1)
            send_bias(0, g, g == sub - 1)

    def project(c, u, lo, width, wq):
        y = mm(u, wq)
        q, k, v, gl = [y[:, i * chan:(i + 1) * chan] for i in range(4)]
        keys[c, pl.ds(lo, width)] = k.astype(BF16)
        gate[c, pl.ds(lo, width)] = jax.nn.sigmoid(gl)
        late = q[width - tail:]
        masked = [jnp.where(even_head, late, 0.0), jnp.where(even_head, 0.0, late)]
        twice = [v[width - tail:], v[width - tail:]]
        if lo == 0:
            qmask[c, :, pl.ds(0, LANES)] = q[:LANES].astype(BF16).T
            v_t[c, :, pl.ds(0, LANES)] = v[:LANES].astype(BF16).T
        if lo + width == seq:
            qmask[c, :, pl.ds(LANES, LANES)] = jnp.concatenate(masked, axis=0).astype(BF16).T
            v_t[c, :, pl.ds(LANES, LANES)] = jnp.concatenate(twice, axis=0).astype(BF16).T

    def spread_start_bias():
        for g in range(sub):
            await_bias(0, g, g == sub - 1)
        for g in range(sub):
            await_twin(0, g)
        for pair in range(heads // 2):
            t0, t1, t2 = [doubled(bias_in[0, :, pair, t].astype(F32).reshape(seq, LANES)).T for t in range(3)]
            even = jnp.concatenate([t0, t2[:tail]], axis=0)
            odd = jnp.concatenate([t1, t2[tail:]], axis=0)
            bias_t[pair, :, pl.ds(0, LANES)] = even[:, :LANES]
            bias_t[pair, :, pl.ds(LANES, LANES)] = odd[:, :LANES]
            bias_t[2, :, pl.ds(pair * LANES, LANES)] = jnp.where(low, even[:, LANES:], odd[:, LANES:])

    def spread_end_bias(lo, count, place):
        for pair in range(heads // 2):
            for t in range(3):
                b = bias_in[1, :, pair, t, pl.ds(lo, count)].astype(F32).reshape(group * count * 8, LANES)
                tile, at = (pair, t * LANES) if t < 2 else (2, pair * LANES)
                bias_t[tile, pl.ds(place, group * count * 8), pl.ds(at, LANES)] = b

    zero = jnp.zeros((dim, LANES), BF16)
    zero2 = jnp.zeros((2 * dim, LANES), BF16)
    zero4 = jnp.zeros((2 * dim, 2 * LANES), BF16)

    def query_tile(r, t):
        if t == 2:
            top = jnp.concatenate([qmask[r, pl.ds(0, 2 * dim), pl.ds(LANES, LANES)], zero2], axis=1)
            bottom = jnp.concatenate([zero2, qmask[r, pl.ds(2 * dim, 2 * dim), pl.ds(LANES, LANES)]], axis=1)
            return jnp.concatenate([top, bottom], axis=0)
        first = qmask[r, pl.ds(2 * t * dim, dim), pl.ds(0, LANES)]
        second = qmask[r, pl.ds((2 * t + 1) * dim, dim), pl.ds(0, LANES)]
        pair = jnp.concatenate([jnp.concatenate([first, zero], axis=1), jnp.concatenate([zero, second], axis=1)], axis=0)
        return jnp.concatenate([pair, zero4] if t == 0 else [zero4, pair], axis=0)

    def score_tile(r, slot, t):
        s = mm(keys[r], query_tile(r, t)) * scale + bias_t[t]
        scores[slot, t] = s
        tops[slot, t] = jnp.max(s, axis=0, keepdims=True)

    def mix_tile(r, slot, t):
        e = jnp.exp(scores[slot, t] - tops[slot, t])
        total = jnp.sum(e, axis=0, keepdims=True)
        values = v_t[r, :, pl.ds(0, seq)] if t == 2 else v_t[r, pl.ds(2 * t * dim, 2 * dim), pl.ds(0, seq)]
        o = mm(values, e.astype(BF16)) * (1.0 / total)
        if t < 2:
            for h in (2 * t, 2 * t + 1):
                mixed[slot, pl.ds(h * dim, dim), pl.ds(0, LANES)] = o[(h % 2) * dim:(h % 2 + 1) * dim, (h % 2) * LANES:(h % 2 + 1) * LANES]
        else:
            for h in range(heads):
                mixed[slot, pl.ds(h * dim, dim), pl.ds(LANES, LANES)] = o[h * dim:(h + 1) * dim, (h // 2) * LANES:(h // 2 + 1) * LANES]

    def merge_heads(r, slot, wo):
        o = mixed[slot].T
        o = jnp.concatenate([o[:LANES], jnp.where(even_head, o[LANES:LANES + tail], o[LANES + tail:])], axis=0)
        return mm((o * gate[r]).astype(BF16), wo)

    def pipeline(stages, send):
        depth, count = len(stages), rows // 2

        def turn(i, active, eager=False):
            for stage in sorted(active, reverse=True):
                for slot in range(2):
                    stages[stage](2 * (i - stage) + slot, slot)
                if eager:
                    send(i, (stage,))
            if not eager:
                send(i, active)

        for i in range(depth):
            turn(i, range(i + 1), True)

        def step(i, carry):
            turn(i, range(depth))
            return carry

        lax.fori_loop(depth, count, step, 0)
        for i in range(count, count + depth - 1):
            turn(i, range(i - count + 1, depth), True)

    def score(r, slot):
        for t in range(3):
            score_tile(r, slot, t)

    def mix(r, slot):
        for t in range(3):
            mix_tile(r, slot, t)

    def send_rows(first, src, dst, sem):
        some = pl.ds(first, SEND)
        dst[me, some] = src[some, pl.ds(me * sub, sub)]
        peers(lambda d: remote(src.at[some, pl.ds(d * sub, sub)], dst.at[me, some], sem(first), d).start())

    def unpack(src, lo, count, base):
        def part(d):
            flat[pl.ds(base + d * count * rows, count * rows), :] = src[d, pl.ds(lo, count)].astype(F32).reshape(count * rows, chan)

        loop(group, part)

    def by_place(vals):
        parts = vals.reshape(group, sub, 8, chan)
        return jnp.concatenate([parts[:, :early // 8].reshape(LANES, chan), parts[:, early // 8:].reshape(tail, chan)], axis=0)

    loads[1].wait()
    load_bias_weight(0, wbs_ref)
    start_norm()
    loads[0].wait()
    loop(rows, lambda r: project(r, norm[r], 0, seq, wqs_ref[...]), 2)
    for load in loads[2:]:
        load.wait()
    load_bias_weight(1, wbe_ref)
    spread_start_bias()

    def start_merge(r, slot):
        z_new = z_ref[r] + merge_heads(r, slot, wos_ref[...])
        out_ref[r] = z_new
        h_out[r] = z_new.astype(BF16).reshape(seq // 8, 8, chan)

    def end_bias(r, slot):
        h = out_ref[r].astype(BF16).astype(F32)
        put_bias(r, w_b[1].astype(BF16), layer_norm(by_place(h)))

    def start_send(i, active):
        if 2 in active:
            send_rows(2 * (i - 2), h_out, h_in, lambda r: h_sem.at[r // early])
        if 3 in active:
            r = 2 * (i - 3)
            if isinstance(r, int):
                if r % 8 == 6:
                    send_bias(1, r // 8, r // 8 == sub - 1)
            else:
                @pl.when(lax.rem(r, 8) == 6)
                def _():
                    send_bias(1, r // 8, False)

    pipeline((score, mix, start_merge, end_bias), start_send)

    for g in range(sub - 1):
        await_bias(1, g, False)
    wait_recv(h_in.at[others, pl.ds(0, early)], h_sem.at[0])
    unpack(h_in, 0, early, 0)

    def end_project(lo, width):
        return lambda c: project(c, layer_norm(flat[pl.ds(lo * rows + c, width, stride=rows), :]), lo, width, wqe_ref[...])

    loop(rows, end_project(0, LANES), 4)
    for g in range(sub - 1):
        await_twin(1, g)
    spread_end_bias(0, early // 8, 0)
    wait_recv(h_in.at[others, pl.ds(early, rows - early)], h_sem.at[1])
    unpack(h_in, early, rows - early, LANES * rows)
    await_bias(1, sub - 1, True)
    await_twin(1, sub - 1)
    spread_end_bias(early // 8, sub - early // 8, LANES)
    late_project = end_project(LANES, tail)
    column = lambda c: flat[pl.ds(c, seq, stride=rows), :]

    def by_owner(vals):
        parts = vals.reshape(seq // 8, 8, chan)
        base = LANES // 8
        order = []
        for d in range(group):
            order.append(parts[d * early // 8:(d + 1) * early // 8])
            order.append(parts[base + d * (sub - early // 8):base + (d + 1) * (sub - early // 8)])
        return jnp.concatenate(order, axis=0)

    def end_merge(c, slot):
        upd = merge_heads(c, slot, woe_ref[...])
        upds[slot] = upd
        normed[slot] = layer_norm(column(c) + upd)

    def transition(c, slot):
        hidden = jnp.maximum(mm(normed[slot], w1_ref[...]).astype(BF16), 0.0)
        d_out[c] = by_owner(upds[slot] + mm(hidden, w2_ref[...])).astype(BF16)

    def end_send(i, active):
        if 4 in active:
            send_rows(2 * (i - 4), d_out, d_in, lambda c: d_sem.at[c // 8])

    pipeline((lambda c, slot: late_project(c), score, mix, end_merge, transition), end_send)
    for g in range(sub):
        wait_recv(d_in.at[others, pl.ds(g * 8, 8)], d_sem.at[g])

        def part(d):
            flat[pl.ds((d * rows + g * 8) * rows, 8 * rows), :] = d_in[d, pl.ds(g * 8, 8)].astype(F32).reshape(8 * rows, chan)

        loop(group, part, 2)

        def final(r):
            for d in range(group):
                at = d * rows + g * 8
                out_ref[r, pl.ds(at, 8), :] = out_ref[r, pl.ds(at, 8), :] + flat[pl.ds(at * rows + r, 8, stride=rows), :]

        loop(rows, final, 4)

    for phase in range(2):
        wait_send(bias_in.at[phase, others])
    wait_send(h_in.at[others])
    wait_send(d_in.at[others])


def solution(mesh):
    axis = 'sp'
    group = mesh.shape[axis]
    row_spec = P(('dp', 'sp'), None, None)

    def local_fn(pair_loc, w_qkvg_s, w_bias_s, w_out_s, w_qkvg_e, w_bias_e, w_out_e, w_one, w_two):
        rows, seq, chan = pair_loc.shape
        heads = w_bias_s.shape[0]
        sub = rows // 8
        packed = 2 * LANES
        weights = (w_qkvg_s, w_bias_s, w_out_s, w_qkvg_e, w_bias_e, w_out_e, w_one, w_two)
        scratch = [pltpu.VMEM(pair_loc.shape, F32)] + [pltpu.VMEM(w.shape, w.dtype) for w in weights] + [
            pltpu.VMEM((rows * seq, chan), F32),
            pltpu.VMEM((rows, seq, chan), BF16),
            pltpu.VMEM((2, 16, chan), F32),
            pltpu.VMEM((rows, chan, packed), BF16),
            pltpu.VMEM((rows, chan, packed), BF16),
            pltpu.VMEM((rows, seq, chan), F32),
            pltpu.VMEM((rows, seq, chan), BF16),
            pltpu.VMEM((heads // 2, 3, rows, LANES), F32),
            pltpu.VMEM((2, heads // 2, 3, sub, 8, LANES), BF16),
            pltpu.VMEM((2, group, heads // 2, 3, sub, 8, LANES), BF16),
            pltpu.VMEM((3, seq, packed), F32),
            pltpu.VMEM((2, 3, seq, packed), F32),
            pltpu.VMEM((2, 3, 1, packed), F32),
            pltpu.VMEM((2, chan, packed), F32),
            pltpu.VMEM((2, seq, chan), F32),
            pltpu.VMEM((2, seq, chan), BF16),
            pltpu.VMEM((rows, seq // 8, 8, chan), BF16),
            pltpu.VMEM((group, rows, sub, 8, chan), BF16),
            pltpu.VMEM((rows, seq // 8, 8, chan), BF16),
            pltpu.VMEM((group, rows, sub, 8, chan), BF16),
            pltpu.SemaphoreType.DMA((sub,)),
            pltpu.SemaphoreType.DMA((len(weights),)),
            pltpu.SemaphoreType.DMA,
            pltpu.SemaphoreType.DMA((2, sub)),
            pltpu.SemaphoreType.DMA((2, sub)),
            pltpu.SemaphoreType.DMA((2,)),
            pltpu.SemaphoreType.DMA((sub,)),
        ]
        return pl.pallas_call(
            functools.partial(kernel, (group, rows, seq, chan, heads, axis)),
            out_shape=jax.ShapeDtypeStruct(pair_loc.shape, F32),
            in_specs=[pl.BlockSpec(memory_space=pltpu.HBM)] * 9,
            out_specs=pl.BlockSpec(memory_space=pltpu.VMEM),
            scratch_shapes=scratch,
            compiler_params=pltpu.CompilerParams(collective_id=0, has_side_effects=True, vmem_limit_bytes=40 * 2 ** 20),
        )(*[pltpu.with_memory_space_constraint(x, pltpu.HBM) for x in (pair_loc, *weights)])

    return jax.shard_map(local_fn, mesh=mesh, in_specs=(row_spec, P(), P(), P(), P(), P(), P(), P(), P()), out_specs=row_spec, check_vma=False)
```

```python
import functools

import jax
import jax.numpy as jnp
from jax import lax
from jax.experimental import pallas as pl
from jax.experimental.pallas import tpu as pltpu
from jax.sharding import PartitionSpec as P

LN_EPS = 1e-5
LANES = 128
F32, BF16 = jnp.float32, jnp.bfloat16


def layer_norm(vals):
    mean = jnp.mean(vals, axis=-1, keepdims=True)
    centered = vals - mean
    var = jnp.mean(centered * centered, axis=-1, keepdims=True)
    return (centered * lax.rsqrt(var + LN_EPS)).astype(BF16)


def mm(lhs, rhs, contract=((1,), (0,))):
    return lax.dot_general(lhs, rhs, (contract, ((), ())), preferred_element_type=F32)


def loop(count, body, unroll=1):
    def step(idx, carry):
        for sub in range(unroll):
            body(idx * unroll + sub)
        return carry

    lax.fori_loop(0, count // unroll, step, 0)


def kernel(cfg, z_hbm, wqs_hbm, wbs_hbm, wos_hbm, wqe_hbm, wbe_hbm, woe_hbm, w1_hbm, w2_hbm, out_ref,
           z_ref, wqs_ref, wbs_ref, wos_ref, wqe_ref, wbe_ref, woe_ref, w1_ref, w2_ref,
           flat, norm, w_b, qmask, v_t, gate, keys, bias_rows, bias_out, bias_in, bias_t, scores, tops, mixed, upds, normed,
           h_out, h_in, d_out, d_in, z_sem, w_sem, out_sem, far_sem, near_sem, h_sem, d_sem):
    group, rows, seq, chan, heads, axis = cfg
    dim = chan // heads
    me = lax.axis_index(axis)
    tail = seq - LANES
    sub = rows // 8
    scale = dim ** -0.5
    early = LANES // group

    loads = []
    pairs = ((wqs_hbm, wqs_ref), (wbs_hbm, wbs_ref), (wos_hbm, wos_ref), (wqe_hbm, wqe_ref),
             (wbe_hbm, wbe_ref), (woe_hbm, woe_ref), (w1_hbm, w1_ref), (w2_hbm, w2_ref))
    z_copy = lambda g: pltpu.make_async_copy(z_hbm.at[pl.ds(g * 8, 8)], z_ref.at[pl.ds(g * 8, 8)], z_sem.at[g])
    for g in range(sub):
        z_copy(g).start()
    for i, (src, dst) in enumerate(pairs):
        loads.append(pltpu.make_async_copy(src, dst, w_sem.at[i]))
    loads[1].start()

    barrier = pltpu.get_barrier_semaphore()
    for off in range(1, group):
        pl.semaphore_signal(barrier, inc=1, device_id={axis: lax.rem(me + off, group)}, device_id_type=pl.DeviceIdType.MESH)

    lane = lax.broadcasted_iota(jnp.int32, (1, LANES), 1)
    low = lane < tail
    even_head = (lane // dim) % 2 == 0

    def doubled(rows_in):
        return jnp.concatenate([rows_in, rows_in[LANES:seq]], axis=0)

    def peers(start):
        for off in sorted(range(1, group), key=lambda o: abs(2 * o - group)):
            start(lax.rem(me + off, group))

    def remote(src, dst, recv, dst_dev):
        return pltpu.make_async_remote_copy(src_ref=src, dst_ref=dst, send_sem=out_sem, recv_sem=recv,
                                            device_id={axis: dst_dev}, device_id_type=pl.DeviceIdType.MESH)

    def wait_recv(part, sem):
        pltpu.make_async_remote_copy(src_ref=part, dst_ref=part, send_sem=out_sem, recv_sem=sem,
                                     device_id={axis: me}, device_id_type=pl.DeviceIdType.MESH).wait_recv()

    def wait_send(part):
        pltpu.make_async_remote_copy(src_ref=part, dst_ref=part, send_sem=out_sem, recv_sem=out_sem,
                                     device_id={axis: me}, device_id_type=pl.DeviceIdType.MESH).wait_send()

    others = pl.ds(0, group - 1)

    def load_bias_weight(phase, wb_ref):
        w_b[phase] = jnp.zeros(w_b.shape[1:], w_b.dtype)
        w_b[phase, pl.ds(0, heads), :] = wb_ref[...].astype(F32)

    def put_bias(r, wb, u):
        b = mm(wb, doubled(u), ((1,), (1,)))
        for pair in range(heads // 2):
            even, odd = b[2 * pair:2 * pair + 1], b[2 * pair + 1:2 * pair + 2]
            bias_rows[pair, 0, pl.ds(r, 1), :] = even[:, :LANES]
            bias_rows[pair, 1, pl.ds(r, 1), :] = odd[:, :LANES]
            bias_rows[pair, 2, pl.ds(r, 1), :] = jnp.where(low, even[:, LANES:], odd[:, LANES:])

    def round_bias(phase, g):
        rounded = bias_rows[:, :, pl.ds(pl.multiple_of(g * 8, 8), 8)].astype(BF16).reshape(heads // 2, 3, 1, 8, LANES)
        bias_out[phase, :, :, pl.ds(g, 1)] = rounded
        bias_in[phase, me, :, :, pl.ds(g, 1)] = rounded

    twin = me + 1 - 2 * lax.rem(me, 2)

    def bias_copy(phase, g, src, slot, sem, d):
        remote(src, bias_in.at[phase, slot, :, :, pl.ds(g, 1)], sem.at[phase, g], d).start()

    def send_bias(phase, g, direct):
        round_bias(phase, g)
        src = bias_out.at[phase, :, :, pl.ds(g, 1)]
        for off in range(1, group):
            if off % 2 == 0:
                bias_copy(phase, g, src, me, far_sem, lax.rem(me + off, group))
            elif direct:
                bias_copy(phase, g, src, me, near_sem, lax.rem(me + off, group))
        if not direct:
            bias_copy(phase, g, src, me, near_sem, twin)

    def await_bias(phase, g, direct):
        wait_recv(bias_in.at[phase, pl.ds(0, group // 2 - 1), :, :, pl.ds(g, 1)], far_sem.at[phase, g])
        if not direct:
            for off in range(2, group, 2):
                slot = lax.rem(me + off, group)
                bias_copy(phase, g, bias_in.at[phase, slot, :, :, pl.ds(g, 1)], slot, near_sem, twin)

    def await_twin(phase, g):
        wait_recv(bias_in.at[phase, pl.ds(0, group // 2), :, :, pl.ds(g, 1)], near_sem.at[phase, g])

    def start_norm():
        wb = w_b[0].astype(BF16)
        for g in range(sub):
            z_copy(g).wait()

            def row(i):
                r = g * 8 + i
                u = layer_norm(z_ref[r])
                norm[r] = u
                put_bias(r, wb, u)

            loop(8, row, 4)
            if g == 0:
                for i, load in enumerate(loads):
                    if i != 1:
                        load.start()
                pl.semaphore_wait(barrier, group - 1)
            send_bias(0, g, True)

    def project(c, u, lo, width, wq):
        y = mm(u, wq)
        q, k, v, gl = [y[:, i * chan:(i + 1) * chan] for i in range(4)]
        keys[c, pl.ds(lo, width)] = k.astype(BF16)
        gate[c, pl.ds(lo, width)] = jax.nn.sigmoid(gl)
        late = q[width - tail:]
        masked = [jnp.where(even_head, late, 0.0), jnp.where(even_head, 0.0, late)]
        twice = [v[width - tail:], v[width - tail:]]
        if lo == 0:
            qmask[c, :, pl.ds(0, LANES)] = q[:LANES].astype(BF16).T
            v_t[c, :, pl.ds(0, LANES)] = v[:LANES].astype(BF16).T
        if lo + width == seq:
            qmask[c, :, pl.ds(LANES, LANES)] = jnp.concatenate(masked, axis=0).astype(BF16).T
            v_t[c, :, pl.ds(LANES, LANES)] = jnp.concatenate(twice, axis=0).astype(BF16).T

    def spread_start_bias():
        for g in range(sub):
            await_bias(0, g, True)
        for g in range(sub):
            await_twin(0, g)
        for pair in range(heads // 2):
            t0, t1, t2 = [doubled(bias_in[0, :, pair, t].astype(F32).reshape(seq, LANES)).T for t in range(3)]
            even = jnp.concatenate([t0, t2[:tail]], axis=0)
            odd = jnp.concatenate([t1, t2[tail:]], axis=0)
            bias_t[pair, :, pl.ds(0, LANES)] = even[:, :LANES]
            bias_t[pair, :, pl.ds(LANES, LANES)] = odd[:, :LANES]
            bias_t[2, :, pl.ds(pair * LANES, LANES)] = jnp.where(low, even[:, LANES:], odd[:, LANES:])

    def spread_end_bias(lo, count, place):
        for pair in range(heads // 2):
            for t in range(3):
                b = bias_in[1, :, pair, t, pl.ds(lo, count)].astype(F32).reshape(group * count * 8, LANES)
                tile, at = (pair, t * LANES) if t < 2 else (2, pair * LANES)
                bias_t[tile, pl.ds(place, group * count * 8), pl.ds(at, LANES)] = b

    zero = jnp.zeros((dim, LANES), BF16)
    zero2 = jnp.zeros((2 * dim, LANES), BF16)
    zero4 = jnp.zeros((2 * dim, 2 * LANES), BF16)

    def query_tile(r, t):
        if t == 2:
            top = jnp.concatenate([qmask[r, pl.ds(0, 2 * dim), pl.ds(LANES, LANES)], zero2], axis=1)
            bottom = jnp.concatenate([zero2, qmask[r, pl.ds(2 * dim, 2 * dim), pl.ds(LANES, LANES)]], axis=1)
            return jnp.concatenate([top, bottom], axis=0)
        first = qmask[r, pl.ds(2 * t * dim, dim), pl.ds(0, LANES)]
        second = qmask[r, pl.ds((2 * t + 1) * dim, dim), pl.ds(0, LANES)]
        pair = jnp.concatenate([jnp.concatenate([first, zero], axis=1), jnp.concatenate([zero, second], axis=1)], axis=0)
        return jnp.concatenate([pair, zero4] if t == 0 else [zero4, pair], axis=0)

    def score_tile(r, slot, t):
        s = mm(keys[r], query_tile(r, t)) * scale + bias_t[t]
        scores[slot, t] = s
        tops[slot, t] = jnp.max(s, axis=0, keepdims=True)

    def mix_tile(r, slot, t):
        e = jnp.exp(scores[slot, t] - tops[slot, t])
        total = jnp.sum(e, axis=0, keepdims=True)
        values = v_t[r, :, pl.ds(0, seq)] if t == 2 else v_t[r, pl.ds(2 * t * dim, 2 * dim), pl.ds(0, seq)]
        o = mm(values, e.astype(BF16)) * (1.0 / total)
        if t < 2:
            for h in (2 * t, 2 * t + 1):
                mixed[slot, pl.ds(h * dim, dim), pl.ds(0, LANES)] = o[(h % 2) * dim:(h % 2 + 1) * dim, (h % 2) * LANES:(h % 2 + 1) * LANES]
        else:
            for h in range(heads):
                mixed[slot, pl.ds(h * dim, dim), pl.ds(LANES, LANES)] = o[h * dim:(h + 1) * dim, (h // 2) * LANES:(h // 2 + 1) * LANES]

    def merge_heads(r, slot, wo):
        o = mixed[slot].T
        o = jnp.concatenate([o[:LANES], jnp.where(even_head, o[LANES:LANES + tail], o[LANES + tail:])], axis=0)
        return mm((o * gate[r]).astype(BF16), wo)

    def pipeline(stages, send, sender, chunk):
        depth, count = len(stages), rows // 2

        def steps(i, parity, stage):
            pair, half = i - stage, (parity + stage) % 2
            return [part for slot in range(2) for part in stages[stage](2 * pair + slot, 2 * half + slot)]

        def turn(i, parity, active):
            light, heavy = [], []
            for stage in active:
                for part in steps(i, parity, stage):
                    (light if stages[stage] in (score, mix) else heavy).append((part, stage))
            light.sort(key=lambda entry: -entry[1])
            mixes = [part for part, stage in light if stages[stage] is mix]
            marks = [part for part, stage in light if stages[stage] is score]
            light = [part for both in zip(mixes, marks) for part in both] if mixes and marks else mixes + marks
            heavy = [part for part, _ in sorted(heavy, key=lambda entry: -entry[1])]
            every = max(1, -(-len(light) // max(1, len(heavy))))
            while light or heavy:
                for part in heavy[:1] + light[:every]:
                    part()
                heavy, light = heavy[1:], light[every:]

        def peeled(i):
            active = [stage for stage in range(depth) if 0 <= i - stage < count]
            if sender in active:
                for part in steps(i, i % 2, sender):
                    part()
                send(i, 2, (sender,))
                active.remove(sender)
            turn(i, i % 2, active)
            send(i, 2, active)

        first = sender + 2
        for i in range(first):
            peeled(i)
        base = first if first >= depth - 1 else depth - 1

        def step(k, carry):
            i = base + 2 * k
            for j in range(2):
                turn(i + j, (base + j) % 2, range(depth))
                if chunk == 2:
                    send(i + j, 2, range(depth))
            if chunk == 4:
                send(i, 4, range(depth))
            return carry

        lax.fori_loop(0, (count - base) // 2, step, 0)
        for i in range(base + (count - base) // 2 * 2, count + depth - 1):
            peeled(i)

    def score(r, slot):
        return [functools.partial(score_tile, r, slot, t) for t in range(3)]

    def mix(r, slot):
        return [functools.partial(mix_tile, r, slot, t) for t in range(3)]

    def send_rows(first, size, src, dst, sem):
        some = pl.ds(first, size)
        dst[me, some] = src[some, pl.ds(me * sub, sub)]
        peers(lambda d: remote(src.at[some, pl.ds(d * sub, sub)], dst.at[me, some], sem(first), d).start())

    def unpack(src, lo, base, stride):
        def part(d):
            flat[pl.ds((base + d * stride) * rows, 8 * rows), :] = src[d, pl.ds(lo, 8)].astype(F32).reshape(8 * rows, chan)

        loop(group, part)

    def by_place(vals):
        parts = vals.reshape(group, sub, 8, chan)
        return jnp.concatenate([parts[:, :early // 8].reshape(LANES, chan), parts[:, early // 8:].reshape(tail, chan)], axis=0)

    loads[1].wait()
    load_bias_weight(0, wbs_ref)
    start_norm()
    loads[0].wait()
    loop(rows, lambda r: project(r, norm[r], 0, seq, wqs_ref[...]), 2)
    for load in loads[2:]:
        load.wait()
    load_bias_weight(1, wbe_ref)
    spread_start_bias()

    def start_merge(r, slot):
        z_new = z_ref[r] + merge_heads(r, slot, wos_ref[...])
        out_ref[r] = z_new
        h_out[r] = z_new.astype(BF16).reshape(seq // 8, 8, chan)

    def end_bias(r, slot):
        h = out_ref[r].astype(BF16).astype(F32)
        put_bias(r, w_b[1].astype(BF16), layer_norm(by_place(h)))

    def start_send(i, size, active):
        if 2 in active:
            send_rows(2 * (i - 2), size, h_out, h_in, lambda r: h_sem.at[r // 8])
        if 3 in active:
            pair = i - 3
            if isinstance(pair, int):
                if pair % 4 == 3:
                    send_bias(1, pair // 4, pair // 4 == sub - 1)
            else:
                @pl.when(lax.rem(pair, 4) == 3)
                def _():
                    send_bias(1, pair // 4, False)

    pipeline((score, mix, lambda r, slot: [lambda: start_merge(r, slot)], lambda r, slot: [lambda: end_bias(r, slot)]), start_send, 2, 4)

    for g in range(sub - 1):
        wait_recv(h_in.at[others, pl.ds(g * 8, 8)], h_sem.at[g])
        unpack(h_in, g * 8, g * 8, early)

    def end_project(lo, width):
        return lambda c: project(c, layer_norm(flat[pl.ds(lo * rows + c, width, stride=rows), :]), lo, width, wqe_ref[...])

    loop(rows, end_project(0, LANES), 4)
    for g in range(sub - 1):
        await_bias(1, g, False)
    wait_recv(h_in.at[others, pl.ds(early, 8)], h_sem.at[sub - 1])
    unpack(h_in, early, LANES, 8)
    for g in range(sub - 1):
        await_twin(1, g)
    spread_end_bias(0, early // 8, 0)
    await_bias(1, sub - 1, True)
    await_twin(1, sub - 1)
    spread_end_bias(early // 8, sub - early // 8, LANES)
    late_project = end_project(LANES, tail)
    column = lambda c: flat[pl.ds(c, seq, stride=rows), :]

    def by_owner(vals):
        parts = vals.reshape(seq // 8, 8, chan)
        base = LANES // 8
        order = []
        for d in range(group):
            order.append(parts[d * early // 8:(d + 1) * early // 8])
            order.append(parts[base + d * (sub - early // 8):base + (d + 1) * (sub - early // 8)])
        return jnp.concatenate(order, axis=0)

    def end_merge(c, slot):
        upd = merge_heads(c, slot, woe_ref[...])
        upds[slot] = upd
        normed[slot] = layer_norm(column(c) + upd)

    def transition(c, slot):
        hidden = jnp.maximum(mm(normed[slot], w1_ref[...]).astype(BF16), 0.0)
        d_out[c] = by_owner(upds[slot] + mm(hidden, w2_ref[...])).astype(BF16)

    def end_send(i, size, active):
        if 4 in active:
            send_rows(2 * (i - 4), size, d_out, d_in, lambda c: d_sem.at[c // 8])

    pipeline((lambda c, slot: [lambda: late_project(c)], score, mix, lambda c, slot: [lambda: end_merge(c, slot)],
              lambda c, slot: [lambda: transition(c, slot)]), end_send, 4, 2)
    for g in range(sub):
        wait_recv(d_in.at[others, pl.ds(g * 8, 8)], d_sem.at[g])

        def part(d):
            flat[pl.ds((d * rows + g * 8) * rows, 8 * rows), :] = d_in[d, pl.ds(g * 8, 8)].astype(F32).reshape(8 * rows, chan)

        loop(group, part, 2)

        def final(r):
            for d in range(group):
                at = d * rows + g * 8
                out_ref[r, pl.ds(at, 8), :] = out_ref[r, pl.ds(at, 8), :] + flat[pl.ds(at * rows + r, 8, stride=rows), :]

        loop(rows, final, 4)

    for phase in range(2):
        wait_send(bias_in.at[phase, others])
    wait_send(h_in.at[others])
    wait_send(d_in.at[others])


def solution(mesh):
    axis = 'sp'
    group = mesh.shape[axis]
    row_spec = P(('dp', 'sp'), None, None)

    def local_fn(pair_loc, w_qkvg_s, w_bias_s, w_out_s, w_qkvg_e, w_bias_e, w_out_e, w_one, w_two):
        rows, seq, chan = pair_loc.shape
        heads = w_bias_s.shape[0]
        sub = rows // 8
        packed = 2 * LANES
        weights = (w_qkvg_s, w_bias_s, w_out_s, w_qkvg_e, w_bias_e, w_out_e, w_one, w_two)
        scratch = [pltpu.VMEM(pair_loc.shape, F32)] + [pltpu.VMEM(w.shape, w.dtype) for w in weights] + [
            pltpu.VMEM((rows * seq, chan), F32),
            pltpu.VMEM((rows, seq, chan), BF16),
            pltpu.VMEM((2, 16, chan), F32),
            pltpu.VMEM((rows, chan, packed), BF16),
            pltpu.VMEM((rows, chan, packed), BF16),
            pltpu.VMEM((rows, seq, chan), F32),
            pltpu.VMEM((rows, seq, chan), BF16),
            pltpu.VMEM((heads // 2, 3, rows, LANES), F32),
            pltpu.VMEM((2, heads // 2, 3, sub, 8, LANES), BF16),
            pltpu.VMEM((2, group, heads // 2, 3, sub, 8, LANES), BF16),
            pltpu.VMEM((3, seq, packed), F32),
            pltpu.VMEM((4, 3, seq, packed), F32),
            pltpu.VMEM((4, 3, 1, packed), F32),
            pltpu.VMEM((4, chan, packed), F32),
            pltpu.VMEM((4, seq, chan), F32),
            pltpu.VMEM((4, seq, chan), BF16),
            pltpu.VMEM((rows, seq // 8, 8, chan), BF16),
            pltpu.VMEM((group, rows, sub, 8, chan), BF16),
            pltpu.VMEM((rows, seq // 8, 8, chan), BF16),
            pltpu.VMEM((group, rows, sub, 8, chan), BF16),
            pltpu.SemaphoreType.DMA((sub,)),
            pltpu.SemaphoreType.DMA((len(weights),)),
            pltpu.SemaphoreType.DMA,
            pltpu.SemaphoreType.DMA((2, sub)),
            pltpu.SemaphoreType.DMA((2, sub)),
            pltpu.SemaphoreType.DMA((sub,)),
            pltpu.SemaphoreType.DMA((sub,)),
        ]
        return pl.pallas_call(
            functools.partial(kernel, (group, rows, seq, chan, heads, axis)),
            out_shape=jax.ShapeDtypeStruct(pair_loc.shape, F32),
            in_specs=[pl.BlockSpec(memory_space=pltpu.HBM)] * 9,
            out_specs=pl.BlockSpec(memory_space=pltpu.VMEM),
            scratch_shapes=scratch,
            compiler_params=pltpu.CompilerParams(collective_id=0, has_side_effects=True, vmem_limit_bytes=40 * 2 ** 20),
        )(*[pltpu.with_memory_space_constraint(x, pltpu.HBM) for x in (pair_loc, *weights)])

    return jax.shard_map(local_fn, mesh=mesh, in_specs=(row_spec, P(), P(), P(), P(), P(), P(), P(), P()), out_specs=row_spec, check_vma=False)
```

```python
import functools

import jax
import jax.numpy as jnp
from jax import lax
from jax.experimental import pallas as pl
from jax.experimental.pallas import tpu as pltpu
from jax.sharding import PartitionSpec as P

LN_EPS = 1e-5
LANES = 128
F32, BF16 = jnp.float32, jnp.bfloat16


def layer_norm(vals):
    mean = jnp.mean(vals, axis=-1, keepdims=True)
    centered = vals - mean
    var = jnp.mean(centered * centered, axis=-1, keepdims=True)
    return (centered * lax.rsqrt(var + LN_EPS)).astype(BF16)


def mm(lhs, rhs, contract=((1,), (0,))):
    return lax.dot_general(lhs, rhs, (contract, ((), ())), preferred_element_type=F32)


def loop(count, body, unroll=1):
    def step(idx, carry):
        for sub in range(unroll):
            body(idx * unroll + sub)
        return carry

    lax.fori_loop(0, count // unroll, step, 0)


def kernel(cfg, z_hbm, wqs_hbm, wbs_hbm, wos_hbm, wqe_hbm, wbe_hbm, woe_hbm, w1_hbm, w2_hbm, out_ref,
           z_ref, wqs_ref, wbs_ref, wos_ref, wqe_ref, wbe_ref, woe_ref, w1_ref, w2_ref,
           flat, norm, w_b, qmask, v_t, gate, keys, bias_rows, bias_out, bias_in, bias_t, scores, tops, mixed, upds, normed,
           h_out, h_in, d_out, d_in, z_sem, w_sem, out_sem, far_sem, near_sem, h_sem, d_sem):
    group, rows, seq, chan, heads, axis = cfg
    dim = chan // heads
    me = lax.axis_index(axis)
    tail = seq - LANES
    sub = rows // 8
    scale = dim ** -0.5
    early = LANES // group

    loads = []
    pairs = ((wqs_hbm, wqs_ref), (wbs_hbm, wbs_ref), (wos_hbm, wos_ref), (wqe_hbm, wqe_ref),
             (wbe_hbm, wbe_ref), (woe_hbm, woe_ref), (w1_hbm, w1_ref), (w2_hbm, w2_ref))
    z_copy = lambda g: pltpu.make_async_copy(z_hbm.at[pl.ds(g * 8, 8)], z_ref.at[pl.ds(g * 8, 8)], z_sem.at[g])
    for g in range(sub):
        z_copy(g).start()
    for i, (src, dst) in enumerate(pairs):
        loads.append(pltpu.make_async_copy(src, dst, w_sem.at[i]))
    loads[1].start()

    barrier = pltpu.get_barrier_semaphore()
    for off in range(1, group):
        pl.semaphore_signal(barrier, inc=1, device_id={axis: lax.rem(me + off, group)}, device_id_type=pl.DeviceIdType.MESH)

    lane = lax.broadcasted_iota(jnp.int32, (1, LANES), 1)
    low = lane < tail
    even_head = (lane // dim) % 2 == 0

    def doubled(rows_in):
        return jnp.concatenate([rows_in, rows_in[LANES:seq]], axis=0)

    def peers(start):
        for off in sorted(range(1, group), key=lambda o: abs(2 * o - group)):
            start(lax.rem(me + off, group))

    def remote(src, dst, recv, dst_dev):
        return pltpu.make_async_remote_copy(src_ref=src, dst_ref=dst, send_sem=out_sem, recv_sem=recv,
                                            device_id={axis: dst_dev}, device_id_type=pl.DeviceIdType.MESH)

    def wait_recv(part, sem):
        pltpu.make_async_remote_copy(src_ref=part, dst_ref=part, send_sem=out_sem, recv_sem=sem,
                                     device_id={axis: me}, device_id_type=pl.DeviceIdType.MESH).wait_recv()

    def wait_send(part):
        pltpu.make_async_remote_copy(src_ref=part, dst_ref=part, send_sem=out_sem, recv_sem=out_sem,
                                     device_id={axis: me}, device_id_type=pl.DeviceIdType.MESH).wait_send()

    others = pl.ds(0, group - 1)

    def load_bias_weight(phase, wb_ref):
        w_b[phase] = jnp.zeros(w_b.shape[1:], w_b.dtype)
        w_b[phase, pl.ds(0, heads), :] = wb_ref[...].astype(F32)

    def put_bias(r, wb, u):
        b = mm(wb, doubled(u), ((1,), (1,)))
        for pair in range(heads // 2):
            even, odd = b[2 * pair:2 * pair + 1], b[2 * pair + 1:2 * pair + 2]
            bias_rows[pair, 0, pl.ds(r, 1), :] = even[:, :LANES]
            bias_rows[pair, 1, pl.ds(r, 1), :] = odd[:, :LANES]
            bias_rows[pair, 2, pl.ds(r, 1), :] = jnp.where(low, even[:, LANES:], odd[:, LANES:])

    def round_bias(phase, g):
        rounded = bias_rows[:, :, pl.ds(pl.multiple_of(g * 8, 8), 8)].astype(BF16).reshape(heads // 2, 3, 1, 8, LANES)
        bias_out[phase, :, :, pl.ds(g, 1)] = rounded
        bias_in[phase, me, :, :, pl.ds(g, 1)] = rounded

    twin = me + 1 - 2 * lax.rem(me, 2)

    def bias_copy(phase, g, src, slot, sem, d):
        remote(src, bias_in.at[phase, slot, :, :, pl.ds(g, 1)], sem.at[phase, g], d).start()

    def send_bias(phase, g, direct):
        round_bias(phase, g)
        src = bias_out.at[phase, :, :, pl.ds(g, 1)]
        for off in range(1, group):
            if off % 2 == 0:
                bias_copy(phase, g, src, me, far_sem, lax.rem(me + off, group))
            elif direct:
                bias_copy(phase, g, src, me, near_sem, lax.rem(me + off, group))
        if not direct:
            bias_copy(phase, g, src, me, near_sem, twin)

    def await_bias(phase, g, direct):
        wait_recv(bias_in.at[phase, pl.ds(0, group // 2 - 1), :, :, pl.ds(g, 1)], far_sem.at[phase, g])
        if not direct:
            for off in range(2, group, 2):
                slot = lax.rem(me + off, group)
                bias_copy(phase, g, bias_in.at[phase, slot, :, :, pl.ds(g, 1)], slot, near_sem, twin)

    def await_twin(phase, g):
        wait_recv(bias_in.at[phase, pl.ds(0, group // 2), :, :, pl.ds(g, 1)], near_sem.at[phase, g])

    def start_norm():
        wb = w_b[0].astype(BF16)
        for g in range(sub):
            z_copy(g).wait()

            def row(i):
                r = g * 8 + i
                u = layer_norm(z_ref[r])
                norm[r] = u
                put_bias(r, wb, u)

            loop(8, row, 4)
            if g == 0:
                for i, load in enumerate(loads):
                    if i != 1:
                        load.start()
                pl.semaphore_wait(barrier, group - 1)
            send_bias(0, g, True)

    def project(c, u, lo, width, wq):
        y = mm(u, wq)
        q, k, v, gl = [y[:, i * chan:(i + 1) * chan] for i in range(4)]
        keys[c, pl.ds(lo, width)] = k.astype(BF16)
        gate[c, pl.ds(lo, width)] = jax.nn.sigmoid(gl)
        late = q[width - tail:]
        masked = [jnp.where(even_head, late, 0.0), jnp.where(even_head, 0.0, late)]
        twice = [v[width - tail:], v[width - tail:]]
        if lo == 0:
            qmask[c, :, pl.ds(0, LANES)] = q[:LANES].astype(BF16).T
            v_t[c, :, pl.ds(0, LANES)] = v[:LANES].astype(BF16).T
        if lo + width == seq:
            qmask[c, :, pl.ds(LANES, LANES)] = jnp.concatenate(masked, axis=0).astype(BF16).T
            v_t[c, :, pl.ds(LANES, LANES)] = jnp.concatenate(twice, axis=0).astype(BF16).T

    def spread_start_bias():
        for g in range(sub):
            await_bias(0, g, True)
        for g in range(sub):
            await_twin(0, g)
        for pair in range(heads // 2):
            t0, t1, t2 = [doubled(bias_in[0, :, pair, t].astype(F32).reshape(seq, LANES)).T for t in range(3)]
            even = jnp.concatenate([t0, t2[:tail]], axis=0)
            odd = jnp.concatenate([t1, t2[tail:]], axis=0)
            bias_t[pair, :, pl.ds(0, LANES)] = even[:, :LANES]
            bias_t[pair, :, pl.ds(LANES, LANES)] = odd[:, :LANES]
            bias_t[2, :, pl.ds(pair * LANES, LANES)] = jnp.where(low, even[:, LANES:], odd[:, LANES:])

    def spread_end_bias(lo, count, place):
        for pair in range(heads // 2):
            for t in range(3):
                b = bias_in[1, :, pair, t, pl.ds(lo, count)].astype(F32).reshape(group * count * 8, LANES)
                tile, at = (pair, t * LANES) if t < 2 else (2, pair * LANES)
                bias_t[tile, pl.ds(place, group * count * 8), pl.ds(at, LANES)] = b

    zero = jnp.zeros((dim, LANES), BF16)
    zero2 = jnp.zeros((2 * dim, LANES), BF16)
    zero4 = jnp.zeros((2 * dim, 2 * LANES), BF16)

    def query_tile(r, t):
        if t == 2:
            top = jnp.concatenate([qmask[r, pl.ds(0, 2 * dim), pl.ds(LANES, LANES)], zero2], axis=1)
            bottom = jnp.concatenate([zero2, qmask[r, pl.ds(2 * dim, 2 * dim), pl.ds(LANES, LANES)]], axis=1)
            return jnp.concatenate([top, bottom], axis=0)
        first = qmask[r, pl.ds(2 * t * dim, dim), pl.ds(0, LANES)]
        second = qmask[r, pl.ds((2 * t + 1) * dim, dim), pl.ds(0, LANES)]
        pair = jnp.concatenate([jnp.concatenate([first, zero], axis=1), jnp.concatenate([zero, second], axis=1)], axis=0)
        return jnp.concatenate([pair, zero4] if t == 0 else [zero4, pair], axis=0)

    def score_tile(r, slot, t):
        s = mm(keys[r], query_tile(r, t)) * scale + bias_t[t]
        scores[slot, t] = s
        tops[slot, t] = jnp.max(s, axis=0, keepdims=True)

    def raw_tiles(rs):
        for slot, r in enumerate(rs):
            for t in range(3):
                scores[slot, t] = mm(keys[r], query_tile(r, t)) * scale

    def biased_tile(slot, t):
        s = scores[slot, t] + bias_t[t]
        scores[slot, t] = s
        tops[slot, t] = jnp.max(s, axis=0, keepdims=True)

    def mix_tile(r, slot, t):
        e = jnp.exp(scores[slot, t] - tops[slot, t])
        total = jnp.sum(e, axis=0, keepdims=True)
        values = v_t[r, :, pl.ds(0, seq)] if t == 2 else v_t[r, pl.ds(2 * t * dim, 2 * dim), pl.ds(0, seq)]
        o = mm(values, e.astype(BF16)) * (1.0 / total)
        if t < 2:
            for h in (2 * t, 2 * t + 1):
                mixed[slot, pl.ds(h * dim, dim), pl.ds(0, LANES)] = o[(h % 2) * dim:(h % 2 + 1) * dim, (h % 2) * LANES:(h % 2 + 1) * LANES]
        else:
            for h in range(heads):
                mixed[slot, pl.ds(h * dim, dim), pl.ds(LANES, LANES)] = o[h * dim:(h + 1) * dim, (h // 2) * LANES:(h // 2 + 1) * LANES]

    def merge_heads(r, slot, wo):
        o = mixed[slot].T
        o = jnp.concatenate([o[:LANES], jnp.where(even_head, o[LANES:LANES + tail], o[LANES + tail:])], axis=0)
        return mm((o * gate[r]).astype(BF16), wo)

    def pipeline(stages, send, sender, chunk, done=()):
        depth, count = len(stages), rows // 2

        def steps(i, parity, stage):
            pair, half = i - stage, (parity + stage) % 2
            if isinstance(pair, int) and (stage, pair) in done:
                return []
            if isinstance(pair, int) and pair == 0 and stages[stage] is score:
                return [functools.partial(biased_tile, slot, t) for slot in range(2) for t in range(3)]
            return [part for slot in range(2) for part in stages[stage](2 * pair + slot, 2 * half + slot)]

        def turn(i, parity, active):
            light, heavy = [], []
            for stage in active:
                for part in steps(i, parity, stage):
                    (light if stages[stage] in (score, mix) else heavy).append((part, stage))
            light.sort(key=lambda entry: -entry[1])
            mixes = [part for part, stage in light if stages[stage] is mix]
            marks = [part for part, stage in light if stages[stage] is score]
            light = [part for both in zip(mixes, marks) for part in both] if mixes and marks else mixes + marks
            heavy = [part for part, _ in sorted(heavy, key=lambda entry: -entry[1])]
            every = max(1, -(-len(light) // max(1, len(heavy))))
            while light or heavy:
                for part in heavy[:1] + light[:every]:
                    part()
                heavy, light = heavy[1:], light[every:]

        def peeled(i):
            active = [stage for stage in range(depth) if 0 <= i - stage < count]
            if sender in active:
                for part in steps(i, i % 2, sender):
                    part()
                send(i, 2, (sender,))
                active.remove(sender)
            turn(i, i % 2, active)
            send(i, 2, active)

        first = sender + 2
        for i in range(first):
            peeled(i)
        base = first if first >= depth - 1 else depth - 1

        def step(k, carry):
            i = base + 2 * k
            for j in range(2):
                turn(i + j, (base + j) % 2, range(depth))
                if chunk == 2:
                    send(i + j, 2, range(depth))
            if chunk == 4:
                send(i, 4, range(depth))
            return carry

        lax.fori_loop(0, (count - base) // 2, step, 0)
        for i in range(base + (count - base) // 2 * 2, count + depth - 1):
            peeled(i)

    def score(r, slot):
        return [functools.partial(score_tile, r, slot, t) for t in range(3)]

    def mix(r, slot):
        return [functools.partial(mix_tile, r, slot, t) for t in range(3)]

    def send_rows(first, size, src, dst, sem):
        some = pl.ds(first, size)
        dst[me, some] = src[some, pl.ds(me * sub, sub)]
        peers(lambda d: remote(src.at[some, pl.ds(d * sub, sub)], dst.at[me, some], sem(first), d).start())

    def unpack(src, lo, base, stride):
        def part(d):
            flat[pl.ds((base + d * stride) * rows, 8 * rows), :] = src[d, pl.ds(lo, 8)].astype(F32).reshape(8 * rows, chan)

        loop(group, part)

    def by_place(vals):
        parts = vals.reshape(group, sub, 8, chan)
        return jnp.concatenate([parts[:, :early // 8].reshape(LANES, chan), parts[:, early // 8:].reshape(tail, chan)], axis=0)

    loads[1].wait()
    load_bias_weight(0, wbs_ref)
    start_norm()
    loads[0].wait()
    loop(rows, lambda r: project(r, norm[r], 0, seq, wqs_ref[...]), 2)
    for load in loads[2:]:
        load.wait()
    load_bias_weight(1, wbe_ref)
    raw_tiles((0, 1))
    spread_start_bias()

    def start_merge(r, slot):
        z_new = z_ref[r] + merge_heads(r, slot, wos_ref[...])
        out_ref[r] = z_new
        h_out[r] = z_new.astype(BF16).reshape(seq // 8, 8, chan)

    def end_bias(r, slot):
        h = out_ref[r].astype(BF16).astype(F32)
        put_bias(r, w_b[1].astype(BF16), layer_norm(by_place(h)))

    def start_send(i, size, active):
        if 2 in active:
            send_rows(2 * (i - 2), size, h_out, h_in, lambda r: h_sem.at[r // 8])
        if 3 in active:
            pair = i - 3
            if isinstance(pair, int):
                if pair % 4 == 3:
                    send_bias(1, pair // 4, pair // 4 == sub - 1)
            else:
                @pl.when(lax.rem(pair, 4) == 3)
                def _():
                    send_bias(1, pair // 4, False)

    pipeline((score, mix, lambda r, slot: [lambda: start_merge(r, slot)], lambda r, slot: [lambda: end_bias(r, slot)]), start_send, 2, 4)

    for g in range(sub - 1):
        wait_recv(h_in.at[others, pl.ds(g * 8, 8)], h_sem.at[g])
        unpack(h_in, g * 8, g * 8, early)

    def end_project(lo, width):
        return lambda c: project(c, layer_norm(flat[pl.ds(lo * rows + c, width, stride=rows), :]), lo, width, wqe_ref[...])

    loop(rows, end_project(0, LANES), 4)
    for g in range(sub - 1):
        await_bias(1, g, False)
    wait_recv(h_in.at[others, pl.ds(early, 8)], h_sem.at[sub - 1])
    unpack(h_in, early, LANES, 8)
    late_project = end_project(LANES, tail)
    for c in range(4):
        late_project(c)
    raw_tiles((0, 1))
    for g in range(sub - 1):
        await_twin(1, g)
    spread_end_bias(0, early // 8, 0)
    await_bias(1, sub - 1, True)
    await_twin(1, sub - 1)
    spread_end_bias(early // 8, sub - early // 8, LANES)
    column = lambda c: flat[pl.ds(c, seq, stride=rows), :]

    def by_owner(vals):
        parts = vals.reshape(seq // 8, 8, chan)
        base = LANES // 8
        order = []
        for d in range(group):
            order.append(parts[d * early // 8:(d + 1) * early // 8])
            order.append(parts[base + d * (sub - early // 8):base + (d + 1) * (sub - early // 8)])
        return jnp.concatenate(order, axis=0)

    def end_merge(c, slot):
        upd = merge_heads(c, slot, woe_ref[...])
        upds[slot] = upd
        normed[slot] = layer_norm(column(c) + upd)

    def transition(c, slot):
        hidden = jnp.maximum(mm(normed[slot], w1_ref[...]).astype(BF16), 0.0)
        d_out[c] = by_owner(upds[slot] + mm(hidden, w2_ref[...])).astype(BF16)

    def end_send(i, size, active):
        if 4 in active:
            send_rows(2 * (i - 4), size, d_out, d_in, lambda c: d_sem.at[c // 8])

    pipeline((lambda c, slot: [lambda: late_project(c)], score, mix, lambda c, slot: [lambda: end_merge(c, slot)],
              lambda c, slot: [lambda: transition(c, slot)]), end_send, 4, 2, ((0, 0), (0, 1)))
    for g in range(sub):
        wait_recv(d_in.at[others, pl.ds(g * 8, 8)], d_sem.at[g])

        def part(d):
            flat[pl.ds((d * rows + g * 8) * rows, 8 * rows), :] = d_in[d, pl.ds(g * 8, 8)].astype(F32).reshape(8 * rows, chan)

        loop(group, part, 2)

        def final(r):
            for d in range(group):
                at = d * rows + g * 8
                out_ref[r, pl.ds(at, 8), :] = out_ref[r, pl.ds(at, 8), :] + flat[pl.ds(at * rows + r, 8, stride=rows), :]

        loop(rows, final, 4)

    for phase in range(2):
        wait_send(bias_in.at[phase, others])
    wait_send(h_in.at[others])
    wait_send(d_in.at[others])


def solution(mesh):
    axis = 'sp'
    group = mesh.shape[axis]
    row_spec = P(('dp', 'sp'), None, None)

    def local_fn(pair_loc, w_qkvg_s, w_bias_s, w_out_s, w_qkvg_e, w_bias_e, w_out_e, w_one, w_two):
        rows, seq, chan = pair_loc.shape
        heads = w_bias_s.shape[0]
        sub = rows // 8
        packed = 2 * LANES
        weights = (w_qkvg_s, w_bias_s, w_out_s, w_qkvg_e, w_bias_e, w_out_e, w_one, w_two)
        scratch = [pltpu.VMEM(pair_loc.shape, F32)] + [pltpu.VMEM(w.shape, w.dtype) for w in weights] + [
            pltpu.VMEM((rows * seq, chan), F32),
            pltpu.VMEM((rows, seq, chan), BF16),
            pltpu.VMEM((2, 16, chan), F32),
            pltpu.VMEM((rows, chan, packed), BF16),
            pltpu.VMEM((rows, chan, packed), BF16),
            pltpu.VMEM((rows, seq, chan), F32),
            pltpu.VMEM((rows, seq, chan), BF16),
            pltpu.VMEM((heads // 2, 3, rows, LANES), F32),
            pltpu.VMEM((2, heads // 2, 3, sub, 8, LANES), BF16),
            pltpu.VMEM((2, group, heads // 2, 3, sub, 8, LANES), BF16),
            pltpu.VMEM((3, seq, packed), F32),
            pltpu.VMEM((4, 3, seq, packed), F32),
            pltpu.VMEM((4, 3, 1, packed), F32),
            pltpu.VMEM((4, chan, packed), F32),
            pltpu.VMEM((4, seq, chan), F32),
            pltpu.VMEM((4, seq, chan), BF16),
            pltpu.VMEM((rows, seq // 8, 8, chan), BF16),
            pltpu.VMEM((group, rows, sub, 8, chan), BF16),
            pltpu.VMEM((rows, seq // 8, 8, chan), BF16),
            pltpu.VMEM((group, rows, sub, 8, chan), BF16),
            pltpu.SemaphoreType.DMA((sub,)),
            pltpu.SemaphoreType.DMA((len(weights),)),
            pltpu.SemaphoreType.DMA,
            pltpu.SemaphoreType.DMA((2, sub)),
            pltpu.SemaphoreType.DMA((2, sub)),
            pltpu.SemaphoreType.DMA((sub,)),
            pltpu.SemaphoreType.DMA((sub,)),
        ]
        return pl.pallas_call(
            functools.partial(kernel, (group, rows, seq, chan, heads, axis)),
            out_shape=jax.ShapeDtypeStruct(pair_loc.shape, F32),
            in_specs=[pl.BlockSpec(memory_space=pltpu.HBM)] * 9,
            out_specs=pl.BlockSpec(memory_space=pltpu.VMEM),
            scratch_shapes=scratch,
            compiler_params=pltpu.CompilerParams(collective_id=0, has_side_effects=True, vmem_limit_bytes=40 * 2 ** 20),
        )(*[pltpu.with_memory_space_constraint(x, pltpu.HBM) for x in (pair_loc, *weights)])

    return jax.shard_map(local_fn, mesh=mesh, in_specs=(row_spec, P(), P(), P(), P(), P(), P(), P(), P()), out_specs=row_spec, check_vma=False)
```

```python
import functools

import jax
import jax.numpy as jnp
from jax import lax
from jax.experimental import pallas as pl
from jax.experimental.pallas import tpu as pltpu
from jax.sharding import PartitionSpec as P

LN_EPS = 1e-5
LANES = 128
F32, BF16 = jnp.float32, jnp.bfloat16


def layer_norm(vals):
    mean = jnp.mean(vals, axis=-1, keepdims=True)
    centered = vals - mean
    var = jnp.mean(centered * centered, axis=-1, keepdims=True)
    return (centered * lax.rsqrt(var + LN_EPS)).astype(BF16)


def mm(lhs, rhs, contract=((1,), (0,))):
    return lax.dot_general(lhs, rhs, (contract, ((), ())), preferred_element_type=F32)


def loop(count, body, unroll=1):
    def step(idx, carry):
        for sub in range(unroll):
            body(idx * unroll + sub)
        return carry

    lax.fori_loop(0, count // unroll, step, 0)


def kernel(cfg, z_hbm, wqs_hbm, wbs_hbm, wos_hbm, wqe_hbm, wbe_hbm, woe_hbm, w1_hbm, w2_hbm, out_ref,
           z_ref, wqs_ref, wbs_ref, wos_ref, wqe_ref, wbe_ref, woe_ref, w1_ref, w2_ref,
           flat, norm, w_b, qmask, v_t, gate, keys, bias_rows, bias_out, bias_in, bias_t, scores, tops, mixed, upds, normed,
           h_out, h_in, d_out, d_in, z_sem, w_sem, out_sem, far_sem, near_sem, h_sem, d_sem):
    group, rows, seq, chan, heads, axis = cfg
    dim = chan // heads
    me = lax.axis_index(axis)
    tail = seq - LANES
    sub = rows // 8
    scale = dim ** -0.5
    early = LANES // group

    loads = []
    pairs = ((wqs_hbm, wqs_ref), (wbs_hbm, wbs_ref), (wos_hbm, wos_ref), (wqe_hbm, wqe_ref),
             (wbe_hbm, wbe_ref), (woe_hbm, woe_ref), (w1_hbm, w1_ref), (w2_hbm, w2_ref))
    z_copy = lambda g: pltpu.make_async_copy(z_hbm.at[pl.ds(g * 8, 8)], z_ref.at[pl.ds(g * 8, 8)], z_sem.at[g])
    for g in range(sub):
        z_copy(g).start()
    for i, (src, dst) in enumerate(pairs):
        loads.append(pltpu.make_async_copy(src, dst, w_sem.at[i]))
    loads[1].start()

    barrier = pltpu.get_barrier_semaphore()
    for off in range(1, group):
        pl.semaphore_signal(barrier, inc=1, device_id={axis: lax.rem(me + off, group)}, device_id_type=pl.DeviceIdType.MESH)

    lane = lax.broadcasted_iota(jnp.int32, (1, LANES), 1)
    low = lane < tail
    even_head = (lane // dim) % 2 == 0

    def doubled(rows_in):
        return jnp.concatenate([rows_in, rows_in[LANES:seq]], axis=0)

    def peers(start):
        for off in sorted(range(1, group), key=lambda o: abs(2 * o - group)):
            start(lax.rem(me + off, group))

    def remote(src, dst, recv, dst_dev):
        return pltpu.make_async_remote_copy(src_ref=src, dst_ref=dst, send_sem=out_sem, recv_sem=recv,
                                            device_id={axis: dst_dev}, device_id_type=pl.DeviceIdType.MESH)

    def wait_recv(part, sem):
        pltpu.make_async_remote_copy(src_ref=part, dst_ref=part, send_sem=out_sem, recv_sem=sem,
                                     device_id={axis: me}, device_id_type=pl.DeviceIdType.MESH).wait_recv()

    def wait_send(part):
        pltpu.make_async_remote_copy(src_ref=part, dst_ref=part, send_sem=out_sem, recv_sem=out_sem,
                                     device_id={axis: me}, device_id_type=pl.DeviceIdType.MESH).wait_send()

    others = pl.ds(0, group - 1)

    def load_bias_weight(phase, wb_ref):
        w_b[phase] = jnp.zeros(w_b.shape[1:], w_b.dtype)
        w_b[phase, pl.ds(0, heads), :] = wb_ref[...].astype(F32)

    def put_bias(r, wb, u):
        b = mm(wb, doubled(u), ((1,), (1,)))
        for pair in range(heads // 2):
            even, odd = b[2 * pair:2 * pair + 1], b[2 * pair + 1:2 * pair + 2]
            bias_rows[pair, 0, pl.ds(r, 1), :] = even[:, :LANES]
            bias_rows[pair, 1, pl.ds(r, 1), :] = odd[:, :LANES]
            bias_rows[pair, 2, pl.ds(r, 1), :] = jnp.where(low, even[:, LANES:], odd[:, LANES:])

    def round_bias(phase, g):
        rounded = bias_rows[:, :, pl.ds(pl.multiple_of(g * 8, 8), 8)].astype(BF16).reshape(heads // 2, 3, 1, 8, LANES)
        bias_out[phase, :, :, pl.ds(g, 1)] = rounded
        bias_in[phase, me, :, :, pl.ds(g, 1)] = rounded

    twin = me + 1 - 2 * lax.rem(me, 2)

    def bias_copy(phase, g, src, slot, sem, d):
        remote(src, bias_in.at[phase, slot, :, :, pl.ds(g, 1)], sem.at[phase, g], d).start()

    def send_bias(phase, g, direct):
        round_bias(phase, g)
        src = bias_out.at[phase, :, :, pl.ds(g, 1)]
        for off in range(1, group):
            if off % 2 == 0:
                bias_copy(phase, g, src, me, far_sem, lax.rem(me + off, group))
            elif direct:
                bias_copy(phase, g, src, me, near_sem, lax.rem(me + off, group))
        if not direct:
            bias_copy(phase, g, src, me, near_sem, twin)

    def await_bias(phase, g, direct):
        wait_recv(bias_in.at[phase, pl.ds(0, group // 2 - 1), :, :, pl.ds(g, 1)], far_sem.at[phase, g])
        if not direct:
            for off in range(2, group, 2):
                slot = lax.rem(me + off, group)
                bias_copy(phase, g, bias_in.at[phase, slot, :, :, pl.ds(g, 1)], slot, near_sem, twin)

    def await_twin(phase, g):
        wait_recv(bias_in.at[phase, pl.ds(0, group // 2), :, :, pl.ds(g, 1)], near_sem.at[phase, g])

    def start_norm():
        wb = w_b[0].astype(BF16)
        for g in range(sub):
            z_copy(g).wait()

            def row(i):
                r = g * 8 + i
                u = layer_norm(z_ref[r])
                norm[r] = u
                put_bias(r, wb, u)

            loop(8, row, 8)
            if g == 0:
                for i, load in enumerate(loads):
                    if i != 1:
                        load.start()
                pl.semaphore_wait(barrier, group - 1)
            send_bias(0, g, True)

    def project(c, u, lo, width, wq):
        y = mm(u, wq)
        q, k, v, gl = [y[:, i * chan:(i + 1) * chan] for i in range(4)]
        keys[c, pl.ds(lo, width)] = k.astype(BF16)
        gate[c, pl.ds(lo, width)] = jax.nn.sigmoid(gl)
        late = q[width - tail:]
        masked = [jnp.where(even_head, late, 0.0), jnp.where(even_head, 0.0, late)]
        twice = [v[width - tail:], v[width - tail:]]
        if lo == 0:
            qmask[c, :, pl.ds(0, LANES)] = q[:LANES].astype(BF16).T
            v_t[c, :, pl.ds(0, LANES)] = v[:LANES].astype(BF16).T
        if lo + width == seq:
            qmask[c, :, pl.ds(LANES, LANES)] = jnp.concatenate(masked, axis=0).astype(BF16).T
            v_t[c, :, pl.ds(LANES, LANES)] = jnp.concatenate(twice, axis=0).astype(BF16).T

    def spread_start_bias():
        for g in range(sub):
            await_bias(0, g, True)
        for g in range(sub):
            await_twin(0, g)
        for pair in range(heads // 2):
            t0, t1, t2 = [doubled(bias_in[0, :, pair, t].astype(F32).reshape(seq, LANES)).T for t in range(3)]
            even = jnp.concatenate([t0, t2[:tail]], axis=0)
            odd = jnp.concatenate([t1, t2[tail:]], axis=0)
            bias_t[pair, :, pl.ds(0, LANES)] = even[:, :LANES]
            bias_t[pair, :, pl.ds(LANES, LANES)] = odd[:, :LANES]
            bias_t[2, :, pl.ds(pair * LANES, LANES)] = jnp.where(low, even[:, LANES:], odd[:, LANES:])

    def spread_end_bias(lo, count, place):
        for pair in range(heads // 2):
            for t in range(3):
                b = bias_in[1, :, pair, t, pl.ds(lo, count)].astype(F32).reshape(group * count * 8, LANES)
                tile, at = (pair, t * LANES) if t < 2 else (2, pair * LANES)
                bias_t[tile, pl.ds(place, group * count * 8), pl.ds(at, LANES)] = b

    zero = jnp.zeros((dim, LANES), BF16)
    zero2 = jnp.zeros((2 * dim, LANES), BF16)
    zero4 = jnp.zeros((2 * dim, 2 * LANES), BF16)

    def query_tile(r, t):
        if t == 2:
            top = jnp.concatenate([qmask[r, pl.ds(0, 2 * dim), pl.ds(LANES, LANES)], zero2], axis=1)
            bottom = jnp.concatenate([zero2, qmask[r, pl.ds(2 * dim, 2 * dim), pl.ds(LANES, LANES)]], axis=1)
            return jnp.concatenate([top, bottom], axis=0)
        first = qmask[r, pl.ds(2 * t * dim, dim), pl.ds(0, LANES)]
        second = qmask[r, pl.ds((2 * t + 1) * dim, dim), pl.ds(0, LANES)]
        pair = jnp.concatenate([jnp.concatenate([first, zero], axis=1), jnp.concatenate([zero, second], axis=1)], axis=0)
        return jnp.concatenate([pair, zero4] if t == 0 else [zero4, pair], axis=0)

    def score_tile(r, slot, t):
        s = mm(keys[r], query_tile(r, t)) * scale + bias_t[t]
        scores[slot, t] = s
        tops[slot, t] = jnp.max(s, axis=0, keepdims=True)

    def raw_tiles(rs):
        for slot, r in enumerate(rs):
            for t in range(3):
                scores[slot, t] = mm(keys[r], query_tile(r, t)) * scale

    def biased_tile(slot, t):
        s = scores[slot, t] + bias_t[t]
        scores[slot, t] = s
        tops[slot, t] = jnp.max(s, axis=0, keepdims=True)

    def mix_tile(r, slot, t):
        e = jnp.exp(scores[slot, t] - tops[slot, t])
        total = jnp.sum(e, axis=0, keepdims=True)
        values = v_t[r, :, pl.ds(0, seq)] if t == 2 else v_t[r, pl.ds(2 * t * dim, 2 * dim), pl.ds(0, seq)]
        o = mm(values, e.astype(BF16)) * (1.0 / total)
        if t < 2:
            for h in (2 * t, 2 * t + 1):
                mixed[slot, pl.ds(h * dim, dim), pl.ds(0, LANES)] = o[(h % 2) * dim:(h % 2 + 1) * dim, (h % 2) * LANES:(h % 2 + 1) * LANES]
        else:
            for h in range(heads):
                mixed[slot, pl.ds(h * dim, dim), pl.ds(LANES, LANES)] = o[h * dim:(h + 1) * dim, (h // 2) * LANES:(h // 2 + 1) * LANES]

    def merge_heads(r, slot, wo):
        o = mixed[slot].T
        o = jnp.concatenate([o[:LANES], jnp.where(even_head, o[LANES:LANES + tail], o[LANES + tail:])], axis=0)
        return mm((o * gate[r]).astype(BF16), wo)

    def pipeline(stages, send, sender, chunk, done=()):
        depth, count = len(stages), rows // 2

        def steps(i, parity, stage):
            pair, half = i - stage, (parity + stage) % 2
            if isinstance(pair, int) and (stage, pair) in done:
                return []
            if isinstance(pair, int) and pair == 0 and stages[stage] is score:
                return [functools.partial(biased_tile, slot, t) for slot in range(2) for t in range(3)]
            return [part for slot in range(2) for part in stages[stage](2 * pair + slot, 2 * half + slot)]

        def turn(i, parity, active):
            light, heavy = [], []
            for stage in active:
                for part in steps(i, parity, stage):
                    (light if stages[stage] in (score, mix) else heavy).append((part, stage))
            light.sort(key=lambda entry: -entry[1])
            mixes = [part for part, stage in light if stages[stage] is mix]
            marks = [part for part, stage in light if stages[stage] is score]
            light = [part for both in zip(mixes, marks) for part in both] if mixes and marks else mixes + marks
            heavy = [part for part, _ in sorted(heavy, key=lambda entry: -entry[1])]
            every = max(1, -(-len(light) // max(1, len(heavy))))
            while light or heavy:
                for part in heavy[:1] + light[:every]:
                    part()
                heavy, light = heavy[1:], light[every:]

        def peeled(i):
            active = [stage for stage in range(depth) if 0 <= i - stage < count]
            if sender in active:
                for part in steps(i, i % 2, sender):
                    part()
                send(i, 2, (sender,))
                active.remove(sender)
            turn(i, i % 2, active)
            send(i, 2, active)

        first = sender + 2
        for i in range(first):
            peeled(i)
        base = first if first >= depth - 1 else depth - 1

        def step(k, carry):
            i = base + 2 * k
            for j in range(2):
                turn(i + j, (base + j) % 2, range(depth))
                if chunk == 2:
                    send(i + j, 2, range(depth))
            if chunk == 4:
                send(i, 4, range(depth))
            return carry

        lax.fori_loop(0, (count - base) // 2, step, 0)
        for i in range(base + (count - base) // 2 * 2, count + depth - 1):
            peeled(i)

    def score(r, slot):
        return [functools.partial(score_tile, r, slot, t) for t in range(3)]

    def mix(r, slot):
        return [functools.partial(mix_tile, r, slot, t) for t in range(3)]

    def send_rows(first, size, src, dst, sem):
        some = pl.ds(first, size)
        dst[me, some] = src[some, pl.ds(me * sub, sub)]
        peers(lambda d: remote(src.at[some, pl.ds(d * sub, sub)], dst.at[me, some], sem(first), d).start())

    def unpack(src, lo, base, stride):
        def part(d):
            flat[pl.ds((base + d * stride) * rows, 8 * rows), :] = src[d, pl.ds(lo, 8)].astype(F32).reshape(8 * rows, chan)

        loop(group, part)

    def by_place(vals):
        parts = vals.reshape(group, sub, 8, chan)
        return jnp.concatenate([parts[:, :early // 8].reshape(LANES, chan), parts[:, early // 8:].reshape(tail, chan)], axis=0)

    loads[1].wait()
    load_bias_weight(0, wbs_ref)
    start_norm()
    loads[0].wait()
    loop(rows, lambda r: project(r, norm[r], 0, seq, wqs_ref[...]), 2)
    for load in loads[2:]:
        load.wait()
    load_bias_weight(1, wbe_ref)
    raw_tiles((0, 1))
    spread_start_bias()

    def start_merge(r, slot):
        z_new = z_ref[r] + merge_heads(r, slot, wos_ref[...])
        out_ref[r] = z_new
        h_out[r] = z_new.astype(BF16).reshape(seq // 8, 8, chan)

    def end_bias(r, slot):
        h = out_ref[r].astype(BF16).astype(F32)
        put_bias(r, w_b[1].astype(BF16), layer_norm(by_place(h)))

    def start_send(i, size, active):
        if 2 in active:
            send_rows(2 * (i - 2), size, h_out, h_in, lambda r: h_sem.at[r // 8])
        if 3 in active:
            pair = i - 3
            if isinstance(pair, int):
                if pair % 4 == 3:
                    send_bias(1, pair // 4, pair // 4 == sub - 1)
            else:
                @pl.when(lax.rem(pair, 4) == 3)
                def _():
                    send_bias(1, pair // 4, False)

    pipeline((score, mix, lambda r, slot: [lambda: start_merge(r, slot)], lambda r, slot: [lambda: end_bias(r, slot)]), start_send, 2, 2)

    for g in range(sub - 1):
        wait_recv(h_in.at[others, pl.ds(g * 8, 8)], h_sem.at[g])
        unpack(h_in, g * 8, g * 8, early)

    def end_project(lo, width):
        return lambda c: project(c, layer_norm(flat[pl.ds(lo * rows + c, width, stride=rows), :]), lo, width, wqe_ref[...])

    loop(rows, end_project(0, LANES), 4)
    for g in range(sub - 1):
        await_bias(1, g, False)
    wait_recv(h_in.at[others, pl.ds(early, 8)], h_sem.at[sub - 1])
    unpack(h_in, early, LANES, 8)
    late_project = end_project(LANES, tail)
    for c in range(4):
        late_project(c)
    raw_tiles((0, 1))
    for g in range(sub - 1):
        await_twin(1, g)
    spread_end_bias(0, early // 8, 0)
    await_bias(1, sub - 1, True)
    await_twin(1, sub - 1)
    spread_end_bias(early // 8, sub - early // 8, LANES)
    column = lambda c: flat[pl.ds(c, seq, stride=rows), :]

    def by_owner(vals):
        parts = vals.reshape(seq // 8, 8, chan)
        base = LANES // 8
        order = []
        for d in range(group):
            order.append(parts[d * early // 8:(d + 1) * early // 8])
            order.append(parts[base + d * (sub - early // 8):base + (d + 1) * (sub - early // 8)])
        return jnp.concatenate(order, axis=0)

    def end_merge(c, slot):
        upd = merge_heads(c, slot, woe_ref[...])
        upds[slot] = upd
        normed[slot] = layer_norm(column(c) + upd)

    def transition(c, slot):
        hidden = jnp.maximum(mm(normed[slot], w1_ref[...]).astype(BF16), 0.0)
        d_out[c] = by_owner(upds[slot] + mm(hidden, w2_ref[...])).astype(BF16)

    def end_send(i, size, active):
        if 4 in active:
            send_rows(2 * (i - 4), size, d_out, d_in, lambda c: d_sem.at[c // 8])

    pipeline((lambda c, slot: [lambda: late_project(c)], score, mix, lambda c, slot: [lambda: end_merge(c, slot)],
              lambda c, slot: [lambda: transition(c, slot)]), end_send, 4, 2, ((0, 0), (0, 1)))
    for g in range(sub):
        wait_recv(d_in.at[others, pl.ds(g * 8, 8)], d_sem.at[g])

        def part(d):
            flat[pl.ds((d * rows + g * 8) * rows, 8 * rows), :] = d_in[d, pl.ds(g * 8, 8)].astype(F32).reshape(8 * rows, chan)

        loop(group, part, 2)

        def final(r):
            for d in range(group):
                at = d * rows + g * 8
                out_ref[r, pl.ds(at, 8), :] = out_ref[r, pl.ds(at, 8), :] + flat[pl.ds(at * rows + r, 8, stride=rows), :]

        loop(rows, final, 4)

    for phase in range(2):
        wait_send(bias_in.at[phase, others])
    wait_send(h_in.at[others])
    wait_send(d_in.at[others])


def solution(mesh):
    axis = 'sp'
    group = mesh.shape[axis]
    row_spec = P(('dp', 'sp'), None, None)

    def local_fn(pair_loc, w_qkvg_s, w_bias_s, w_out_s, w_qkvg_e, w_bias_e, w_out_e, w_one, w_two):
        rows, seq, chan = pair_loc.shape
        heads = w_bias_s.shape[0]
        sub = rows // 8
        packed = 2 * LANES
        weights = (w_qkvg_s, w_bias_s, w_out_s, w_qkvg_e, w_bias_e, w_out_e, w_one, w_two)
        scratch = [pltpu.VMEM(pair_loc.shape, F32)] + [pltpu.VMEM(w.shape, w.dtype) for w in weights] + [
            pltpu.VMEM((rows * seq, chan), F32),
            pltpu.VMEM((rows, seq, chan), BF16),
            pltpu.VMEM((2, 16, chan), F32),
            pltpu.VMEM((rows, chan, packed), BF16),
            pltpu.VMEM((rows, chan, packed), BF16),
            pltpu.VMEM((rows, seq, chan), F32),
            pltpu.VMEM((rows, seq, chan), BF16),
            pltpu.VMEM((heads // 2, 3, rows, LANES), F32),
            pltpu.VMEM((2, heads // 2, 3, sub, 8, LANES), BF16),
            pltpu.VMEM((2, group, heads // 2, 3, sub, 8, LANES), BF16),
            pltpu.VMEM((3, seq, packed), F32),
            pltpu.VMEM((4, 3, seq, packed), F32),
            pltpu.VMEM((4, 3, 1, packed), F32),
            pltpu.VMEM((4, chan, packed), F32),
            pltpu.VMEM((4, seq, chan), F32),
            pltpu.VMEM((4, seq, chan), BF16),
            pltpu.VMEM((rows, seq // 8, 8, chan), BF16),
            pltpu.VMEM((group, rows, sub, 8, chan), BF16),
            pltpu.VMEM((rows, seq // 8, 8, chan), BF16),
            pltpu.VMEM((group, rows, sub, 8, chan), BF16),
            pltpu.SemaphoreType.DMA((sub,)),
            pltpu.SemaphoreType.DMA((len(weights),)),
            pltpu.SemaphoreType.DMA,
            pltpu.SemaphoreType.DMA((2, sub)),
            pltpu.SemaphoreType.DMA((2, sub)),
            pltpu.SemaphoreType.DMA((sub,)),
            pltpu.SemaphoreType.DMA((sub,)),
        ]
        return pl.pallas_call(
            functools.partial(kernel, (group, rows, seq, chan, heads, axis)),
            out_shape=jax.ShapeDtypeStruct(pair_loc.shape, F32),
            in_specs=[pl.BlockSpec(memory_space=pltpu.HBM)] * 9,
            out_specs=pl.BlockSpec(memory_space=pltpu.VMEM),
            scratch_shapes=scratch,
            compiler_params=pltpu.CompilerParams(collective_id=0, has_side_effects=True, vmem_limit_bytes=40 * 2 ** 20),
        )(*[pltpu.with_memory_space_constraint(x, pltpu.HBM) for x in (pair_loc, *weights)])

    return jax.shard_map(local_fn, mesh=mesh, in_specs=(row_spec, P(), P(), P(), P(), P(), P(), P(), P()), out_specs=row_spec, check_vma=False)
```

```python
import functools

import jax
import jax.numpy as jnp
from jax import lax
from jax.experimental import pallas as pl
from jax.experimental.pallas import tpu as pltpu
from jax.sharding import PartitionSpec as P

LN_EPS = 1e-5
LANES = 128
F32, BF16 = jnp.float32, jnp.bfloat16


def layer_norm(vals):
    mean = jnp.mean(vals, axis=-1, keepdims=True)
    centered = vals - mean
    var = jnp.mean(centered * centered, axis=-1, keepdims=True)
    return (centered * lax.rsqrt(var + LN_EPS)).astype(BF16)


def mm(lhs, rhs, contract=((1,), (0,))):
    return lax.dot_general(lhs, rhs, (contract, ((), ())), preferred_element_type=F32)


def loop(count, body, unroll=1):
    def step(idx, carry):
        for sub in range(unroll):
            body(idx * unroll + sub)
        return carry

    lax.fori_loop(0, count // unroll, step, 0)


def kernel(cfg, z_hbm, wqs_hbm, wbs_hbm, wos_hbm, wqe_hbm, wbe_hbm, woe_hbm, w1_hbm, w2_hbm, out_ref,
           z_ref, wqs_ref, wbs_ref, wos_ref, wqe_ref, wbe_ref, woe_ref, w1_ref, w2_ref,
           flat, norm, w_b, qmask, v_t, gate, keys, bias_rows, bias_out, bias_in, bias_t, scores, tops, mixed, upds, normed,
           h_out, h_in, d_out, d_in, z_sem, w_sem, out_sem, far_sem, near_sem, h_sem, d_sem):
    group, rows, seq, chan, heads, axis = cfg
    dim = chan // heads
    me = lax.axis_index(axis)
    tail = seq - LANES
    sub = rows // 8
    scale = dim ** -0.5
    early = LANES // group

    loads = []
    pairs = ((wqs_hbm, wqs_ref), (wbs_hbm, wbs_ref), (wos_hbm, wos_ref), (wqe_hbm, wqe_ref),
             (wbe_hbm, wbe_ref), (woe_hbm, woe_ref), (w1_hbm, w1_ref), (w2_hbm, w2_ref))
    z_copy = lambda g: pltpu.make_async_copy(z_hbm.at[pl.ds(g * 8, 8)], z_ref.at[pl.ds(g * 8, 8)], z_sem.at[g])
    for g in range(sub):
        z_copy(g).start()
    for i, (src, dst) in enumerate(pairs):
        loads.append(pltpu.make_async_copy(src, dst, w_sem.at[i]))
    loads[1].start()

    barrier = pltpu.get_barrier_semaphore()
    for off in range(1, group):
        pl.semaphore_signal(barrier, inc=1, device_id={axis: lax.rem(me + off, group)}, device_id_type=pl.DeviceIdType.MESH)

    lane = lax.broadcasted_iota(jnp.int32, (1, LANES), 1)
    low = lane < tail
    even_head = (lane // dim) % 2 == 0

    def doubled(rows_in):
        return jnp.concatenate([rows_in, rows_in[LANES:seq]], axis=0)

    def peers(start):
        for off in sorted(range(1, group), key=lambda o: abs(2 * o - group)):
            start(lax.rem(me + off, group))

    def remote(src, dst, recv, dst_dev):
        return pltpu.make_async_remote_copy(src_ref=src, dst_ref=dst, send_sem=out_sem, recv_sem=recv,
                                            device_id={axis: dst_dev}, device_id_type=pl.DeviceIdType.MESH)

    def wait_recv(part, sem):
        pltpu.make_async_remote_copy(src_ref=part, dst_ref=part, send_sem=out_sem, recv_sem=sem,
                                     device_id={axis: me}, device_id_type=pl.DeviceIdType.MESH).wait_recv()

    def wait_send(part):
        pltpu.make_async_remote_copy(src_ref=part, dst_ref=part, send_sem=out_sem, recv_sem=out_sem,
                                     device_id={axis: me}, device_id_type=pl.DeviceIdType.MESH).wait_send()

    others = pl.ds(0, group - 1)

    def load_bias_weight(phase, wb_ref):
        w_b[phase] = jnp.zeros(w_b.shape[1:], w_b.dtype)
        w_b[phase, pl.ds(0, heads), :] = wb_ref[...].astype(F32)

    def put_bias(r, wb, u):
        b = mm(wb, doubled(u), ((1,), (1,)))
        for pair in range(heads // 2):
            even, odd = b[2 * pair:2 * pair + 1], b[2 * pair + 1:2 * pair + 2]
            bias_rows[pair, 0, pl.ds(r, 1), :] = even[:, :LANES]
            bias_rows[pair, 1, pl.ds(r, 1), :] = odd[:, :LANES]
            bias_rows[pair, 2, pl.ds(r, 1), :] = jnp.where(low, even[:, LANES:], odd[:, LANES:])

    def round_bias(phase, g):
        rounded = bias_rows[:, :, pl.ds(pl.multiple_of(g * 8, 8), 8)].astype(BF16).reshape(heads // 2, 3, 1, 8, LANES)
        bias_out[phase, :, :, pl.ds(g, 1)] = rounded
        bias_in[phase, me, :, :, pl.ds(g, 1)] = rounded

    twin = me + 1 - 2 * lax.rem(me, 2)

    def bias_copy(phase, g, src, slot, sem, d):
        remote(src, bias_in.at[phase, slot, :, :, pl.ds(g, 1)], sem.at[phase, g], d).start()

    def send_bias(phase, g, direct):
        round_bias(phase, g)
        src = bias_out.at[phase, :, :, pl.ds(g, 1)]
        for off in range(1, group):
            if off % 2 == 0:
                bias_copy(phase, g, src, me, far_sem, lax.rem(me + off, group))
            elif direct:
                bias_copy(phase, g, src, me, near_sem, lax.rem(me + off, group))
        if not direct:
            bias_copy(phase, g, src, me, near_sem, twin)

    def await_bias(phase, g, direct):
        wait_recv(bias_in.at[phase, pl.ds(0, group // 2 - 1), :, :, pl.ds(g, 1)], far_sem.at[phase, g])
        if not direct:
            for off in range(2, group, 2):
                slot = lax.rem(me + off, group)
                bias_copy(phase, g, bias_in.at[phase, slot, :, :, pl.ds(g, 1)], slot, near_sem, twin)

    def await_twin(phase, g):
        wait_recv(bias_in.at[phase, pl.ds(0, group // 2), :, :, pl.ds(g, 1)], near_sem.at[phase, g])

    def start_norm():
        wb = w_b[0].astype(BF16)
        for g in range(sub):
            z_copy(g).wait()

            def row(i):
                r = g * 8 + i
                u = layer_norm(z_ref[r])
                norm[r] = u
                put_bias(r, wb, u)

            loop(8, row, 8)
            if g == 0:
                for i, load in enumerate(loads):
                    if i != 1:
                        load.start()
                pl.semaphore_wait(barrier, group - 1)
            send_bias(0, g, True)

    def project(c, u, lo, width, wq):
        y = mm(u, wq)
        q, k, v, gl = [y[:, i * chan:(i + 1) * chan] for i in range(4)]
        keys[c, pl.ds(lo, width)] = k.astype(BF16)
        gate[c, pl.ds(lo, width)] = jax.nn.sigmoid(gl)
        late = q[width - tail:]
        masked = [jnp.where(even_head, late, 0.0), jnp.where(even_head, 0.0, late)]
        twice = [v[width - tail:], v[width - tail:]]
        if lo == 0:
            qmask[c, :, pl.ds(0, LANES)] = q[:LANES].astype(BF16).T
            v_t[c, :, pl.ds(0, LANES)] = v[:LANES].astype(BF16).T
        if lo + width == seq:
            qmask[c, :, pl.ds(LANES, LANES)] = jnp.concatenate(masked, axis=0).astype(BF16).T
            v_t[c, :, pl.ds(LANES, LANES)] = jnp.concatenate(twice, axis=0).astype(BF16).T

    def spread_start_bias():
        for g in range(sub):
            await_bias(0, g, True)
        for g in range(sub):
            await_twin(0, g)
        for pair in range(heads // 2):
            t0, t1, t2 = [doubled(bias_in[0, :, pair, t].astype(F32).reshape(seq, LANES)).T for t in range(3)]
            even = jnp.concatenate([t0, t2[:tail]], axis=0)
            odd = jnp.concatenate([t1, t2[tail:]], axis=0)
            bias_t[pair, :, pl.ds(0, LANES)] = even[:, :LANES]
            bias_t[pair, :, pl.ds(LANES, LANES)] = odd[:, :LANES]
            bias_t[2, :, pl.ds(pair * LANES, LANES)] = jnp.where(low, even[:, LANES:], odd[:, LANES:])

    def spread_end_bias(lo, count, place):
        for pair in range(heads // 2):
            for t in range(3):
                b = bias_in[1, :, pair, t, pl.ds(lo, count)].astype(F32).reshape(group * count * 8, LANES)
                tile, at = (pair, t * LANES) if t < 2 else (2, pair * LANES)
                bias_t[tile, pl.ds(place, group * count * 8), pl.ds(at, LANES)] = b

    zero = jnp.zeros((dim, LANES), BF16)
    zero2 = jnp.zeros((2 * dim, LANES), BF16)
    zero4 = jnp.zeros((2 * dim, 2 * LANES), BF16)

    def query_tile(r, t):
        if t == 2:
            top = jnp.concatenate([qmask[r, pl.ds(0, 2 * dim), pl.ds(LANES, LANES)], zero2], axis=1)
            bottom = jnp.concatenate([zero2, qmask[r, pl.ds(2 * dim, 2 * dim), pl.ds(LANES, LANES)]], axis=1)
            return jnp.concatenate([top, bottom], axis=0)
        first = qmask[r, pl.ds(2 * t * dim, dim), pl.ds(0, LANES)]
        second = qmask[r, pl.ds((2 * t + 1) * dim, dim), pl.ds(0, LANES)]
        pair = jnp.concatenate([jnp.concatenate([first, zero], axis=1), jnp.concatenate([zero, second], axis=1)], axis=0)
        return jnp.concatenate([pair, zero4] if t == 0 else [zero4, pair], axis=0)

    def score_tile(r, slot, t):
        s = mm(keys[r], query_tile(r, t)) * scale + bias_t[t]
        scores[slot, t] = s
        tops[slot, t] = jnp.max(s, axis=0, keepdims=True)

    def raw_tiles(rs):
        for slot, r in enumerate(rs):
            for t in range(3):
                scores[slot, t] = mm(keys[r], query_tile(r, t)) * scale

    def biased_tile(slot, t):
        s = scores[slot, t] + bias_t[t]
        scores[slot, t] = s
        tops[slot, t] = jnp.max(s, axis=0, keepdims=True)

    def mix_tile(r, slot, t):
        e = jnp.exp(scores[slot, t] - tops[slot, t])
        total = jnp.sum(e, axis=0, keepdims=True)
        values = v_t[r, :, pl.ds(0, seq)] if t == 2 else v_t[r, pl.ds(2 * t * dim, 2 * dim), pl.ds(0, seq)]
        o = mm(values, e.astype(BF16)) * (1.0 / total)
        if t < 2:
            for h in (2 * t, 2 * t + 1):
                mixed[slot, pl.ds(h * dim, dim), pl.ds(0, LANES)] = o[(h % 2) * dim:(h % 2 + 1) * dim, (h % 2) * LANES:(h % 2 + 1) * LANES]
        else:
            for h in range(heads):
                mixed[slot, pl.ds(h * dim, dim), pl.ds(LANES, LANES)] = o[h * dim:(h + 1) * dim, (h // 2) * LANES:(h // 2 + 1) * LANES]

    def merge_heads(r, slot, wo):
        o = mixed[slot].T
        o = jnp.concatenate([o[:LANES], jnp.where(even_head, o[LANES:LANES + tail], o[LANES + tail:])], axis=0)
        return mm((o * gate[r]).astype(BF16), wo)

    def pipeline(stages, send, sender, chunk, done=()):
        depth, count = len(stages), rows // 2

        def steps(i, parity, stage):
            pair, half = i - stage, (parity + stage) % 2
            if isinstance(pair, int) and (stage, pair) in done:
                return []
            if isinstance(pair, int) and pair == 0 and stages[stage] is score:
                return [functools.partial(biased_tile, slot, t) for slot in range(2) for t in range(3)]
            return [part for slot in range(2) for part in stages[stage](2 * pair + slot, 2 * half + slot)]

        def turn(i, parity, active):
            light, heavy = [], []
            for stage in active:
                for part in steps(i, parity, stage):
                    (light if stages[stage] in (score, mix) else heavy).append((part, stage))
            light.sort(key=lambda entry: -entry[1])
            mixes = [part for part, stage in light if stages[stage] is mix]
            marks = [part for part, stage in light if stages[stage] is score]
            light = [part for both in zip(mixes, marks) for part in both] if mixes and marks else mixes + marks
            heavy = [part for part, _ in sorted(heavy, key=lambda entry: -entry[1])]
            every = max(1, -(-len(light) // max(1, len(heavy))))
            while light or heavy:
                for part in heavy[:1] + light[:every]:
                    part()
                heavy, light = heavy[1:], light[every:]

        def peeled(i):
            active = [stage for stage in range(depth) if 0 <= i - stage < count]
            if sender in active:
                for part in steps(i, i % 2, sender):
                    part()
                send(i, 2, (sender,))
                active.remove(sender)
            turn(i, i % 2, active)
            send(i, 2, active)

        first = sender + 2
        for i in range(first):
            peeled(i)
        base = first if first >= depth - 1 else depth - 1

        def step(k, carry):
            i = base + 2 * k
            for j in range(2):
                turn(i + j, (base + j) % 2, range(depth))
                if chunk == 2:
                    send(i + j, 2, range(depth))
            if chunk == 4:
                send(i, 4, range(depth))
            return carry

        lax.fori_loop(0, (count - base) // 2, step, 0)
        for i in range(base + (count - base) // 2 * 2, count + depth - 1):
            peeled(i)

    def score(r, slot):
        return [functools.partial(score_tile, r, slot, t) for t in range(3)]

    def mix(r, slot):
        return [functools.partial(mix_tile, r, slot, t) for t in range(3)]

    def send_rows(first, size, src, dst, sem):
        some = pl.ds(first, size)
        dst[me, some] = src[some, pl.ds(me * sub, sub)]
        peers(lambda d: remote(src.at[some, pl.ds(d * sub, sub)], dst.at[me, some], sem(first), d).start())

    def unpack(src, lo, base, stride):
        def part(d):
            flat[pl.ds((base + d * stride) * rows, 8 * rows), :] = src[d, pl.ds(lo, 8)].astype(F32).reshape(8 * rows, chan)

        loop(group, part, 4)

    def by_place(vals):
        parts = vals.reshape(group, sub, 8, chan)
        return jnp.concatenate([parts[:, :early // 8].reshape(LANES, chan), parts[:, early // 8:].reshape(tail, chan)], axis=0)

    loads[1].wait()
    load_bias_weight(0, wbs_ref)
    start_norm()
    loads[0].wait()
    loop(rows, lambda r: project(r, norm[r], 0, seq, wqs_ref[...]), 2)
    for load in loads[2:]:
        load.wait()
    load_bias_weight(1, wbe_ref)
    raw_tiles((0, 1))
    spread_start_bias()

    def start_merge(r, slot):
        z_new = z_ref[r] + merge_heads(r, slot, wos_ref[...])
        out_ref[r] = z_new
        h_out[r] = z_new.astype(BF16).reshape(seq // 8, 8, chan)

    def end_bias(r, slot):
        h = out_ref[r].astype(BF16).astype(F32)
        put_bias(r, w_b[1].astype(BF16), layer_norm(by_place(h)))

    def start_send(i, size, active):
        if 2 in active:
            send_rows(2 * (i - 2), size, h_out, h_in, lambda r: h_sem.at[r // 8])
        if 3 in active:
            pair = i - 3
            if isinstance(pair, int):
                if pair % 4 == 3:
                    send_bias(1, pair // 4, pair // 4 == sub - 1)
            else:
                @pl.when(lax.rem(pair, 4) == 3)
                def _():
                    send_bias(1, pair // 4, False)

    pipeline((score, mix, lambda r, slot: [lambda: start_merge(r, slot)], lambda r, slot: [lambda: end_bias(r, slot)]), start_send, 2, 2)

    for g in range(sub - 1):
        wait_recv(h_in.at[others, pl.ds(g * 8, 8)], h_sem.at[g])
        unpack(h_in, g * 8, g * 8, early)

    def end_project(lo, width):
        return lambda c: project(c, layer_norm(flat[pl.ds(lo * rows + c, width, stride=rows), :]), lo, width, wqe_ref[...])

    loop(rows, end_project(0, LANES), 4)
    for g in range(sub - 1):
        await_bias(1, g, False)
    wait_recv(h_in.at[others, pl.ds(early, 8)], h_sem.at[sub - 1])
    unpack(h_in, early, LANES, 8)
    late_project = end_project(LANES, tail)
    for c in range(4):
        late_project(c)
    raw_tiles((0, 1))
    for g in range(sub - 1):
        await_twin(1, g)
    spread_end_bias(0, early // 8, 0)
    await_bias(1, sub - 1, True)
    await_twin(1, sub - 1)
    spread_end_bias(early // 8, sub - early // 8, LANES)
    column = lambda c: flat[pl.ds(c, seq, stride=rows), :]

    def by_owner(vals):
        parts = vals.reshape(seq // 8, 8, chan)
        base = LANES // 8
        order = []
        for d in range(group):
            order.append(parts[d * early // 8:(d + 1) * early // 8])
            order.append(parts[base + d * (sub - early // 8):base + (d + 1) * (sub - early // 8)])
        return jnp.concatenate(order, axis=0)

    def end_merge(c, slot):
        upd = merge_heads(c, slot, woe_ref[...])
        upds[slot] = upd
        normed[slot] = layer_norm(column(c) + upd)

    def transition(c, slot):
        hidden = jnp.maximum(mm(normed[slot], w1_ref[...]).astype(BF16), 0.0)
        d_out[c] = by_owner(upds[slot] + mm(hidden, w2_ref[...])).astype(BF16)

    def end_send(i, size, active):
        if 4 in active:
            send_rows(2 * (i - 4), size, d_out, d_in, lambda c: d_sem.at[c // 8])

    pipeline((lambda c, slot: [lambda: late_project(c)], score, mix, lambda c, slot: [lambda: end_merge(c, slot)],
              lambda c, slot: [lambda: transition(c, slot)]), end_send, 4, 2, ((0, 0), (0, 1)))
    for g in range(sub):
        wait_recv(d_in.at[others, pl.ds(g * 8, 8)], d_sem.at[g])

        def part(d):
            flat[pl.ds((d * rows + g * 8) * rows, 8 * rows), :] = d_in[d, pl.ds(g * 8, 8)].astype(F32).reshape(8 * rows, chan)

        loop(group, part, 4)

        def final(r):
            for d in range(group):
                at = d * rows + g * 8
                out_ref[r, pl.ds(at, 8), :] = out_ref[r, pl.ds(at, 8), :] + flat[pl.ds(at * rows + r, 8, stride=rows), :]

        loop(rows, final, 8)

    for phase in range(2):
        wait_send(bias_in.at[phase, others])
    wait_send(h_in.at[others])
    wait_send(d_in.at[others])


def solution(mesh):
    axis = 'sp'
    group = mesh.shape[axis]
    row_spec = P(('dp', 'sp'), None, None)

    def local_fn(pair_loc, w_qkvg_s, w_bias_s, w_out_s, w_qkvg_e, w_bias_e, w_out_e, w_one, w_two):
        rows, seq, chan = pair_loc.shape
        heads = w_bias_s.shape[0]
        sub = rows // 8
        packed = 2 * LANES
        weights = (w_qkvg_s, w_bias_s, w_out_s, w_qkvg_e, w_bias_e, w_out_e, w_one, w_two)
        scratch = [pltpu.VMEM(pair_loc.shape, F32)] + [pltpu.VMEM(w.shape, w.dtype) for w in weights] + [
            pltpu.VMEM((rows * seq, chan), F32),
            pltpu.VMEM((rows, seq, chan), BF16),
            pltpu.VMEM((2, 16, chan), F32),
            pltpu.VMEM((rows, chan, packed), BF16),
            pltpu.VMEM((rows, chan, packed), BF16),
            pltpu.VMEM((rows, seq, chan), F32),
            pltpu.VMEM((rows, seq, chan), BF16),
            pltpu.VMEM((heads // 2, 3, rows, LANES), F32),
            pltpu.VMEM((2, heads // 2, 3, sub, 8, LANES), BF16),
            pltpu.VMEM((2, group, heads // 2, 3, sub, 8, LANES), BF16),
            pltpu.VMEM((3, seq, packed), F32),
            pltpu.VMEM((4, 3, seq, packed), F32),
            pltpu.VMEM((4, 3, 1, packed), F32),
            pltpu.VMEM((4, chan, packed), F32),
            pltpu.VMEM((4, seq, chan), F32),
            pltpu.VMEM((4, seq, chan), BF16),
            pltpu.VMEM((rows, seq // 8, 8, chan), BF16),
            pltpu.VMEM((group, rows, sub, 8, chan), BF16),
            pltpu.VMEM((rows, seq // 8, 8, chan), BF16),
            pltpu.VMEM((group, rows, sub, 8, chan), BF16),
            pltpu.SemaphoreType.DMA((sub,)),
            pltpu.SemaphoreType.DMA((len(weights),)),
            pltpu.SemaphoreType.DMA,
            pltpu.SemaphoreType.DMA((2, sub)),
            pltpu.SemaphoreType.DMA((2, sub)),
            pltpu.SemaphoreType.DMA((sub,)),
            pltpu.SemaphoreType.DMA((sub,)),
        ]
        return pl.pallas_call(
            functools.partial(kernel, (group, rows, seq, chan, heads, axis)),
            out_shape=jax.ShapeDtypeStruct(pair_loc.shape, F32),
            in_specs=[pl.BlockSpec(memory_space=pltpu.HBM)] * 9,
            out_specs=pl.BlockSpec(memory_space=pltpu.VMEM),
            scratch_shapes=scratch,
            compiler_params=pltpu.CompilerParams(collective_id=0, has_side_effects=True, vmem_limit_bytes=40 * 2 ** 20),
        )(*[pltpu.with_memory_space_constraint(x, pltpu.HBM) for x in (pair_loc, *weights)])

    return jax.shard_map(local_fn, mesh=mesh, in_specs=(row_spec, P(), P(), P(), P(), P(), P(), P(), P()), out_specs=row_spec, check_vma=False)
```
